128 devices in a mesh: gx: 4 (over x), gy: 4 (over z_hi, core), gz: 8 (over y, z_lo).
Axes of the slice: x: 4, y: 4, z: 4 (z_hi: 2, z_lo: 2; z = z_hi * 2 + z_lo), core: 2. Of those that a mesh axis runs over, the one named last changes fastest.
Arguments:
- amplitudes: bfloat16 [2, 65536, 2048], P(None, ('gx', 'gy', 'gz')), may hold values from -6 to 6
- pauli_x: int32 [200], replicated, may hold values from 0 to 2047, as said below
- pauli_z: int32 [200], replicated, may hold values from 0 to 2047
- pauli_phase: int32 [200], replicated, may hold values from 0 to 3
Outputs:
- density_real: float32 [2048, 2048], P(('gx', 'gy', 'gz'))
- density_imag: float32 [2048, 2048], P(('gx', 'gy', 'gz'))
- expectations: float32 [2, 200], replicated
The draws below stay inside these ranges and needn't reach their ends.
Inputs may be any that keep to these rules, and one draw needn't show every extreme that they name: Bit q of the mask acts on kept qubit q (the bit of weight 2^q of the last index); pauli_x and pauli_z of a term are never both zero.
All inputs are finite; a program needn't handle non-finite values.
Results may differ from the reference program's by a relative error of at most 0.0003.
Values sent between devices are 32-bit elements; how exact they have to be, the bound alone decides.
No kernel may reach another device: no remote copies, remote signals or barrier semaphores. Data moves between devices by JAX's collectives and lax.ppermute only.
A program may use at most 192 MiB of HBM per device.

```python
import jax
import jax.numpy as jnp
from jax import lax

QUBITS = 11
R = 2048
COLS_ALL = 65536
TERMS = 200


def pauli_masks(key):
    flips = jax.random.randint(jax.random.fold_in(key, 11), (TERMS,), 0, R).astype(jnp.int32)
    phases = jax.random.randint(jax.random.fold_in(key, 23), (TERMS,), 0, R).astype(jnp.int32)
    both_zero = jnp.logical_and(flips == 0, phases == 0)
    phases = jnp.where(both_zero, jnp.int32(1), phases)
    return (flips, phases)


def draw_pauli_x(key, part):
    return pauli_masks(key)[0]


def draw_pauli_z(key, part):
    return pauli_masks(key)[1]


def with_ends(result, key, low, top_value):
    shape = result.shape
    index_at = [jax.random.randint(jax.random.fold_in(key, axis), (), 0, shape[axis]) for axis in range(len(shape))]
    result = result.at[tuple(index_at)].set(low)
    longest = shape.index(max(shape))
    index_at[longest] = (index_at[longest] + 1) % shape[longest]
    return result.at[tuple(index_at)].set(top_value)


def shard_levels(key, extent, cuts, low, high):
    gain, own = 1.0, jax.random.fold_in(key, 6)
    for position, parts in cuts:
        heights = jnp.exp(jax.random.uniform(jax.random.fold_in(own, position), (parts,), jnp.float32, low / len(cuts), high / len(cuts)))
        gain = gain * jnp.repeat(heights, extent[position] // parts).reshape([-1 if axis == position else 1 for axis in range(len(extent))])
    return gain


def bell_draw(stream_key, extent, width, limit, shards=(), kind=jnp.bfloat16):
    array = width * jax.random.normal(stream_key, extent, jnp.float32)
    if shards:
        array = array * shard_levels(stream_key, extent, shards, -0.22, 0.18)
    return jnp.clip(array, -limit, limit).astype(kind)


def setup_inputs(seed: int = 0) -> dict:
    streams_of = jax.random.split(jax.random.key(seed), 5)
    return {
        "amplitudes": bell_draw(streams_of[0], (2, COLS_ALL, R), 1.0, 6.0, ((1, 128),)),
        "pauli_x": draw_pauli_x(jax.random.fold_in(streams_of[4], 71), 0),
        "pauli_z": draw_pauli_z(jax.random.fold_in(streams_of[4], 71), 0),
        "pauli_phase": with_ends(jax.random.randint(streams_of[3], (TERMS,), 0, 4), jax.random.fold_in(streams_of[3], 1), 0, 3).astype(jnp.int32),
    }


def parity_sign(values, masks):
    anded = jnp.bitwise_and(values, masks)
    counted = jnp.zeros_like(anded)
    for bit_index in range(QUBITS):
        counted = counted + jnp.bitwise_and(jnp.right_shift(anded, bit_index), 1)
    return (1 - 2 * jnp.bitwise_and(counted, 1)).astype(jnp.float32)


def phase_parts(pauli_phase):
    phase_real = jnp.where(pauli_phase == 0, 1.0, jnp.where(pauli_phase == 2, -1.0, 0.0)).astype(jnp.float32)
    phase_imag = jnp.where(pauli_phase == 1, 1.0, jnp.where(pauli_phase == 3, -1.0, 0.0)).astype(jnp.float32)
    return phase_real, phase_imag


def reference(amplitudes, pauli_x, pauli_z, pauli_phase):
    real_part = amplitudes[0].astype(jnp.float32)
    imag_part = amplitudes[1].astype(jnp.float32)
    dims = (((0,), (0,)), ((), ()))
    high = lax.Precision.HIGHEST
    gram_real = lax.dot_general(real_part, real_part, dims, precision=high) + lax.dot_general(imag_part, imag_part, dims, precision=high)
    gram_imag = lax.dot_general(imag_part, real_part, dims, precision=high) - lax.dot_general(real_part, imag_part, dims, precision=high)
    total_cols = amplitudes.shape[1]
    density_real = gram_real / total_cols
    density_imag = gram_imag / total_cols
    row_ids = jnp.arange(R, dtype=jnp.int32)[None, :]
    partner = jnp.bitwise_xor(row_ids, pauli_x[:, None])
    picked_real = jnp.take_along_axis(density_real, partner.T, axis=1).T
    picked_imag = jnp.take_along_axis(density_imag, partner.T, axis=1).T
    signs = parity_sign(row_ids, pauli_z[:, None])
    phase_real, phase_imag = phase_parts(pauli_phase)
    sum_real = jnp.sum(signs * picked_real, axis=1)
    sum_imag = jnp.sum(signs * picked_imag, axis=1)
    expect_real = phase_real * sum_real - phase_imag * sum_imag
    expect_imag = phase_real * sum_imag + phase_imag * sum_real
    return density_real, density_imag, jnp.stack([expect_real, expect_imag], 0)
```

```python
import functools

import jax
import jax.numpy as jnp
from jax import lax
from jax.experimental import pallas as pl
from jax.experimental.pallas import tpu as pltpu
from jax.sharding import Mesh
from jax.sharding import PartitionSpec as P

QUBITS = 11
AX = ("gx", "gy_0", "gy_1", "gz_0", "gz_1")
RING = ("gx", "gz_0", ("gy_0", "gz_1"))
CORE = "gy_1"
TILE = 256
COLOURS = (((0, 1, 2), (0, 1, 2)), ((3, 4, 5), (1, 2, 0)), ((6, 7), (2, 0, 1)))


def row_of(x, y, z):
    return x * 256 + (z >> 1) * 128 + y * 32 + (z & 1) * 16


def transpose_kernel(pos_ref, a_ref, out_ref, *, flip):
    core = pos_ref[3] ^ flip
    for block in range(8):
        cols = pl.ds(pl.multiple_of(block * 256 + core * 128, 128), 128)
        re = a_ref[0, :, cols].T
        im = a_ref[1, :, cols].T
        rows = pl.ds(block * 128, 128)
        out_ref[rows, 0:512] = re
        out_ref[rows, 512:1024] = im
        out_ref[rows, 1024:1536] = -re


def transposed(pos, amps, flip):
    return pl.pallas_call(
        functools.partial(transpose_kernel, flip=flip),
        out_shape=jax.ShapeDtypeStruct((1024, 1536), jnp.bfloat16),
        grid_spec=pltpu.PrefetchScalarGridSpec(
            num_scalar_prefetch=1,
            grid=(1,),
            in_specs=[pl.BlockSpec((2, 512, 2048), lambda i, p: (0, 0, 0))],
            out_specs=pl.BlockSpec((1024, 1536), lambda i, p: (0, 0)),
        ),
        compiler_params=pltpu.CompilerParams(vmem_limit_bytes=24 * 2**20),
        cost_estimate=pl.CostEstimate(flops=2 * 10**9, bytes_accessed=7 * 2**20, transcendentals=0),
        name="transposed",
    )(pos, amps)


def gram_tile(lt_ref, w, res_ref, tile, core):
    if tile < 7:
        below = lt_ref[(tile + 1) * 128 :, 0:1024]
        res_ref[(tile + 1) * 128 :, :] = jnp.dot(below, w, preferred_element_type=jnp.float32)
    if tile > 0:
        above = lt_ref[: tile * 128, 512:1536]
        res_ref[: tile * 128, :] = jnp.dot(above, w, preferred_element_type=jnp.float32)
    here = slice(tile * 128, (tile + 1) * 128)
    real = jnp.dot(lt_ref[here, 0:1024], w, preferred_element_type=jnp.float32)
    imag = jnp.dot(lt_ref[here, 512:1536], w, preferred_element_type=jnp.float32)
    row = lax.broadcasted_iota(jnp.int32, (128, TILE), 0) + core * 128
    col = lax.broadcasted_iota(jnp.int32, (128, TILE), 1)
    res_ref[here, :] = jnp.where(row >= col, real, imag)


def other_kernel(pos_ref, lt_ref, w_ref, out_ref, res_ref, *, tiles, order):
    core = pos_ref[3] ^ 1
    for t, tile in enumerate(tiles):
        cols = slice(t * TILE, (t + 1) * TILE)
        w = w_ref[:, :, cols].reshape(1024, TILE)
        gram_tile(lt_ref, w, res_ref, tile, core)
        for x in range(4):
            for y in range(4):
                for z in range(4):
                    k = [(v - pos_ref[n]) & 3 for n, v in enumerate((x, y, z))]
                    row = row_of(x, y, z)
                    out_ref[k[order[0]], k[order[1]], k[order[2]], :, cols] = res_ref[row : row + 16, :]


def own_kernel(pos_ref, lt_ref, w_ref, recv_ref, *refs, tiles, order):
    outs, res_ref = refs[:4], refs[4]
    core = pos_ref[3]
    for t, tile in enumerate(tiles):
        cols = slice(t * TILE, (t + 1) * TILE)
        w = w_ref[:, :, cols].reshape(1024, TILE)
        gram_tile(lt_ref, w, res_ref, tile, core)
        for k0 in range(4):
            for v1 in range(4):
                for v2 in range(4):
                    v0 = (pos_ref[order[0]] + k0) & 3
                    k1 = (v1 - pos_ref[order[1]]) & 3
                    k2 = (v2 - pos_ref[order[2]]) & 3
                    xyz = [None] * 3
                    for n, v in zip(order, (v0, v1, v2)):
                        xyz[n] = v
                    row = pl.multiple_of(row_of(*xyz), 16)
                    outs[k0][k1, k2, :, cols] = res_ref[pl.ds(row, 16), :] + recv_ref[k0, k1, k2, :, cols]


def gram_part(pos, lt, amps, colour, recv=None):
    tiles, order = colour
    width = len(tiles) * TILE
    index = tiles[0] * TILE // width
    whole = pl.BlockSpec((4, 4, 4, 16, width), lambda i, p: (0, 0, 0, 0, 0))
    piece = pl.BlockSpec((4, 4, 16, width), lambda i, p: (0, 0, 0, 0))
    in_specs = [
        pl.BlockSpec((1024, 1536), lambda i, p: (0, 0)),
        pl.BlockSpec((2, 512, width), lambda i, p: (0, 0, index)),
    ]
    if recv is None:
        body, out_specs, args = other_kernel, whole, (pos, lt, amps)
        out_shape = jax.ShapeDtypeStruct((4, 4, 4, 16, width), jnp.float32)
    else:
        body, out_specs, args = own_kernel, [piece] * 4, (pos, lt, amps, recv)
        in_specs.append(whole)
        out_shape = [jax.ShapeDtypeStruct((4, 4, 16, width), jnp.float32)] * 4
    return pl.pallas_call(
        functools.partial(body, tiles=tiles, order=order),
        out_shape=out_shape,
        grid_spec=pltpu.PrefetchScalarGridSpec(
            num_scalar_prefetch=1,
            grid=(1,),
            in_specs=in_specs,
            out_specs=out_specs,
            scratch_shapes=[pltpu.VMEM((1024, TILE), jnp.float32)],
        ),
        compiler_params=pltpu.CompilerParams(vmem_limit_bytes=32 * 2**20),
        cost_estimate=pl.CostEstimate(
            flops=2 * 1024 * 1024 * width, bytes_accessed=2**20 * 8, transcendentals=0
        ),
        name="other" if recv is None else "own",
    )(*args)


def shifted(array, ring, step):
    return lax.ppermute(array, ring, [(i, (i + step) % 4) for i in range(4)])


def exchanged(pieces, ring):
    arrived = {k: shifted(pieces[k], ring, k) for k in (2, 1, 3)}
    return [pieces[0], arrived[1], arrived[2], arrived[3]]


def parity_sign(values, masks):
    anded = jnp.bitwise_and(values, masks)
    for shift in (8, 4, 2, 1):
        anded = jnp.bitwise_xor(anded, jnp.right_shift(anded, shift))
    return (1 - 2 * jnp.bitwise_and(anded, 1)).astype(jnp.float32)


def phase_parts(pauli_phase):
    real = jnp.where(pauli_phase == 0, 1.0, jnp.where(pauli_phase == 2, -1.0, 0.0))
    imag = jnp.where(pauli_phase == 1, 1.0, jnp.where(pauli_phase == 3, -1.0, 0.0))
    return real.astype(jnp.float32), imag.astype(jnp.float32)


def pauli_kernel(first_ref, w_ref, x_ref, z_ref, out_ref):
    terms = x_ref.shape[1]
    rows = lax.broadcasted_iota(jnp.int32, (16, terms), 0) + first_ref[0]
    partner = jnp.bitwise_xor(rows, x_ref[...])
    lane = jnp.bitwise_and(partner, 127)
    block = jnp.right_shift(partner, 7)
    for half in range(terms // 128):
        cols = slice(half * 128, (half + 1) * 128)
        picked = jnp.zeros((16, 128), jnp.float32)
        for b in range(16):
            got = jnp.take_along_axis(w_ref[:, b * 128 : (b + 1) * 128], lane[:, cols], axis=1)
            picked = jnp.where(block[:, cols] == b, got, picked)
        x, z = x_ref[:, cols], z_ref[:, cols]
        row, col = rows[:, cols], partner[:, cols]
        wanted = parity_sign(x, z)
        found = jnp.where(col <= row, 1.0, -1.0)
        twice = jnp.where(x == 0, 1.0, 2.0)
        terms_here = jnp.where(found == wanted, parity_sign(row, z) * picked, 0.0)
        out_ref[:, cols] = twice * jnp.sum(terms_here, axis=0, keepdims=True)


def pauli_parts(first_row, w_rows, x, z):
    return pl.pallas_call(
        pauli_kernel,
        out_shape=jax.ShapeDtypeStruct((1, 256), jnp.float32),
        grid_spec=pltpu.PrefetchScalarGridSpec(
            num_scalar_prefetch=1,
            grid=(1,),
            in_specs=[
                pl.BlockSpec((16, 2048), lambda i, p: (0, 0)),
                pl.BlockSpec((1, 256), lambda i, p: (0, 0)),
                pl.BlockSpec((1, 256), lambda i, p: (0, 0)),
            ],
            out_specs=pl.BlockSpec((1, 256), lambda i, p: (0, 0)),
        ),
        name="pauli",
    )(first_row, w_rows, x, z)


def on_device(amplitudes, pauli_x, pauli_z, pauli_phase):
    total_cols = amplitudes.shape[1] * 128
    pos = jnp.stack(
        [lax.axis_index(RING[0]), lax.axis_index(RING[1]), lax.axis_index(RING[2]), lax.axis_index(CORE)]
    ).astype(jnp.int32)
    lt_other = transposed(pos, amplitudes, 1)
    sent = [gram_part(pos, lt_other, amplitudes, c) for c in COLOURS]
    swapped = [lax.ppermute(s, CORE, [(0, 1), (1, 0)]) for s in sent]
    lt_own = transposed(pos, amplitudes, 0)
    rows = []
    for colour, recv in zip(COLOURS, swapped):
        order = colour[1]
        pieces = gram_part(pos, lt_own, amplitudes, colour, recv)
        a, b, c, d = exchanged(pieces, RING[order[0]])
        pieces = [(a[k] + b[k]) + (c[k] + d[k]) for k in range(4)]
        a, b, c, d = exchanged(pieces, RING[order[1]])
        pieces = [(a[k] + b[k]) + (c[k] + d[k]) for k in range(4)]
        a, b, c, d = exchanged(pieces, RING[order[2]])
        rows.append((a + b) + (c + d))
    w_rows = jnp.concatenate(rows, 1) * (1.0 / total_cols)
    first_row = lax.axis_index(AX) * 16
    x = jnp.pad(pauli_x, (0, 56))[None]
    z = jnp.pad(pauli_z, (0, 56))[None]
    parts = pauli_parts(first_row.astype(jnp.int32)[None], w_rows, x, z)
    blocks = w_rows.reshape(16, 128, 16).transpose(1, 2, 0).reshape(128, 256)
    message = jnp.concatenate([blocks, jnp.broadcast_to(parts, (128, 256))], 1).reshape(128, 4, 128)
    arrived = lax.all_to_all(message, AX, split_axis=0, concat_axis=0, tiled=True)
    w_cols = arrived[:, :2].reshape(128, 16, 16).transpose(1, 0, 2).reshape(16, 2048)
    sums = arrived[:, 2:].sum(0).reshape(256)[:200]
    row = first_row + jnp.arange(16, dtype=jnp.int32)[:, None]
    col = jnp.arange(2048, dtype=jnp.int32)[None]
    density_real = jnp.where(col <= row, w_rows, w_cols)
    density_imag = jnp.where(col > row, w_rows, jnp.where(col < row, -w_cols, 0.0))
    even = parity_sign(pauli_x, pauli_z) > 0
    sum_real = jnp.where(even, sums, 0.0)
    sum_imag = jnp.where(even, 0.0, sums)
    phase_real, phase_imag = phase_parts(pauli_phase)
    expectations = jnp.stack(
        [phase_real * sum_real - phase_imag * sum_imag, phase_real * sum_imag + phase_imag * sum_real], 0
    )
    return density_real, density_imag, expectations


def solution(mesh):
    finer = Mesh(mesh.devices.reshape(mesh.shape["gx"], 2, 2, 4, 2), AX)
    in_specs = (P(None, AX, None), P(), P(), P())
    out_specs = (P(AX, None), P(AX, None), P())
    return jax.shard_map(on_device, mesh=finer, in_specs=in_specs, out_specs=out_specs, check_vma=False)
```

```python
import functools

import jax
import jax.numpy as jnp
from jax import lax
from jax.experimental import pallas as pl
from jax.experimental.pallas import tpu as pltpu
from jax.sharding import Mesh
from jax.sharding import PartitionSpec as P

AX = ("gx", "gy_0", "gy_1", "gz_0", "gz_1")
CORE = "gy_1"
SAME_CORE = ("gx", "gy_0", "gz_0", "gz_1")
CHUNK = 512


def device_index(x, y, z, core):
    return x * 32 + (z >> 1) * 16 + core * 8 + y * 2 + (z & 1)


def ring_perm(turn, step):
    pairs = []
    for x in range(4):
        for y in range(4):
            for z in range(4):
                for core in range(2):
                    to = [x, y, z]
                    axis = (turn + core) % 3
                    to[axis] = (to[axis] + step) % 4
                    pairs.append((device_index(x, y, z, core), device_index(*to, core)))
    return pairs


def round_ring(array, turn, step):
    return lax.ppermute(array, AX, ring_perm(turn, step))


def swapped(array):
    return lax.ppermute(array, CORE, [(0, 1), (1, 0)])


def prepare_kernel(pos_ref, a_ref, lt_ref, own_ref, other_ref):
    core = pos_ref[3]
    for block in range(16):
        cols = slice(block * 128, (block + 1) * 128)
        re = a_ref[0, :, cols].T
        im = a_ref[1, :, cols].T
        lt_ref[cols, 0:512] = re
        lt_ref[cols, 512:1024] = im
        lt_ref[cols, 1024:1536] = -re
    for block in range(8):
        cols = slice(block * 128, (block + 1) * 128)
        for ref, which in ((own_ref, core), (other_ref, core ^ 1)):
            from_cols = pl.ds(pl.multiple_of(block * 256 + which * 128, 128), 128)
            ref[:, cols] = a_ref[:, :, from_cols].reshape(1024, 128)


def prepare(pos, amps):
    return pl.pallas_call(
        prepare_kernel,
        out_shape=[
            jax.ShapeDtypeStruct((2048, 1536), jnp.bfloat16),
            jax.ShapeDtypeStruct((1024, 1024), jnp.bfloat16),
            jax.ShapeDtypeStruct((1024, 1024), jnp.bfloat16),
        ],
        grid_spec=pltpu.PrefetchScalarGridSpec(
            num_scalar_prefetch=1,
            grid=(1,),
            in_specs=[pl.BlockSpec((2, 512, 2048), lambda i, p: (0, 0, 0))],
            out_specs=[
                pl.BlockSpec((2048, 1536), lambda i, p: (0, 0)),
                pl.BlockSpec((1024, 1024), lambda i, p: (0, 0)),
                pl.BlockSpec((1024, 1024), lambda i, p: (0, 0)),
            ],
        ),
        compiler_params=pltpu.CompilerParams(vmem_limit_bytes=20 * 2**20),
        cost_estimate=pl.CostEstimate(flops=2 * 10**9, bytes_accessed=14 * 2**20, transcendentals=0),
        name="prepare",
    )(pos, amps)


CHUNKS = (((2, 0), (2, 1)), ((1, 1), (3, 0)), ((1, 0), (3, 1)), ((0, 0), (0, 1)))


def chunk_kernel(pos_ref, lt_ref, w_ref, *refs, halves, own, waits):
    refs = refs[waits:]
    recv_ref = refs[0] if own else None
    *outs, rows_ref, ids_ref = refs[1:] if own else refs
    whose = pos_ref[3] if own else pos_ref[3] ^ 1
    lane = lax.broadcasted_iota(jnp.int32, (16, 128), 0)
    at = 0
    for k1, half in halves:
        for k2 in (2 * half, 2 * half + 1):
            for k3 in range(4):
                ahead = [(k1, k2, k3), (k3, k1, k2)]
                x, y, z = [
                    (pos_ref[n] + jnp.where(whose == 0, ahead[0][n], ahead[1][n])) & 3 for n in range(3)
                ]
                base = x * 512 + (z >> 1) * 256 + y * 32 + (z & 1) * 16
                for co in range(2):
                    row = pl.multiple_of(base + co * 128, 16)
                    rows_ref[at : at + 16, :] = lt_ref[pl.ds(row, 16), :]
                    ids_ref[at : at + 16, :] = lane + row
                    at += 16
    for tile in range(4):
        cols = slice(tile * 256, (tile + 1) * 256)
        real = jnp.dot(rows_ref[:, 0:1024], w_ref[:, cols], preferred_element_type=jnp.float32)
        imag = jnp.dot(rows_ref[:, 512:1536], w_ref[:, cols], preferred_element_type=jnp.float32)
        for part in range(2):
            here = slice(part * 128, (part + 1) * 128)
            to = slice(tile * 256 + part * 128, tile * 256 + (part + 1) * 128)
            col = lax.broadcasted_iota(jnp.int32, (CHUNK, 128), 1) + ((tile * 2 + part) * 256 + whose * 128)
            value = jnp.where(ids_ref[...] >= col, real[:, here], imag[:, here])
            if own:
                value = value + recv_ref[:, to]
                outs[0][:, to] = value[: CHUNK // 2]
                outs[1][:, to] = value[CHUNK // 2 :]
            else:
                outs[0][:, to] = value


def chunk_part(pos, lt, w, halves, recv=None, waits=()):
    own = recv is not None
    full = pl.BlockSpec((CHUNK, 1024), lambda i, p: (0, 0))
    half = pl.BlockSpec((CHUNK // 2, 1024), lambda i, p: (0, 0))
    args = (pos, lt, w, *waits) + ((recv,) if own else ())
    in_specs = [
        pl.BlockSpec((2048, 1536), lambda i, p: (0, 0)),
        pl.BlockSpec((1024, 1024), lambda i, p: (0, 0)),
        *[pl.BlockSpec(memory_space=pl.ANY) for _ in waits],
    ]
    if own:
        in_specs.append(full)
        out_shape = [jax.ShapeDtypeStruct((CHUNK // 2, 1024), jnp.float32)] * 2
    else:
        out_shape = jax.ShapeDtypeStruct((CHUNK, 1024), jnp.float32)
    return pl.pallas_call(
        functools.partial(chunk_kernel, halves=halves, own=own, waits=len(waits)),
        out_shape=out_shape,
        grid_spec=pltpu.PrefetchScalarGridSpec(
            num_scalar_prefetch=1,
            grid=(1,),
            in_specs=in_specs,
            out_specs=[half] * 2 if own else full,
            scratch_shapes=[pltpu.VMEM((CHUNK, 1536), jnp.bfloat16), pltpu.VMEM((CHUNK, 128), jnp.int32)],
        ),
        compiler_params=pltpu.CompilerParams(vmem_limit_bytes=20 * 2**20),
        cost_estimate=pl.CostEstimate(
            flops=4 * CHUNK * 1024 * 1024, bytes_accessed=2**20 * 8, transcendentals=0
        ),
        name="own" if own else "other",
    )(*args)


def parity_sign(values, masks):
    anded = jnp.bitwise_and(values, masks)
    for shift in (8, 4, 2, 1):
        anded = jnp.bitwise_xor(anded, jnp.right_shift(anded, shift))
    return (1 - 2 * jnp.bitwise_and(anded, 1)).astype(jnp.float32)


def phase_parts(pauli_phase):
    real = jnp.where(pauli_phase == 0, 1.0, jnp.where(pauli_phase == 2, -1.0, 0.0))
    imag = jnp.where(pauli_phase == 1, 1.0, jnp.where(pauli_phase == 3, -1.0, 0.0))
    return real.astype(jnp.float32), imag.astype(jnp.float32)


def pauli_kernel(at_ref, w_ref, x_ref, z_ref, out_ref):
    own = lax.broadcasted_iota(jnp.int32, (32, 128), 0)
    row = at_ref[0] + jnp.where(own >= 16, own + 112, own)
    for half in range(2):
        cols = slice(half * 128, (half + 1) * 128)
        x, z = x_ref[:, cols], z_ref[:, cols]
        col = jnp.bitwise_xor(row, x)
        lane = jnp.bitwise_and(col, 127)
        block = jnp.right_shift(col, 7)
        picked = jnp.zeros((32, 128), jnp.float32)
        for b in range(8):
            got = jnp.take_along_axis(w_ref[:, b * 128 : (b + 1) * 128], lane, axis=1)
            picked = jnp.where(block == 2 * b + at_ref[1], got, picked)
        found = jnp.where(col <= row, 1.0, -1.0)
        twice = jnp.where(x == 0, 1.0, 2.0)
        here = jnp.where(found == parity_sign(x, z), parity_sign(row, z) * picked, 0.0)
        out_ref[:, cols] = twice * jnp.sum(here, axis=0, keepdims=True)


def pauli_parts(at, w_part, x, z):
    return pl.pallas_call(
        pauli_kernel,
        out_shape=jax.ShapeDtypeStruct((1, 256), jnp.float32),
        grid_spec=pltpu.PrefetchScalarGridSpec(
            num_scalar_prefetch=1,
            grid=(1,),
            in_specs=[
                pl.BlockSpec((32, 1024), lambda i, p: (0, 0)),
                pl.BlockSpec((1, 256), lambda i, p: (0, 0)),
                pl.BlockSpec((1, 256), lambda i, p: (0, 0)),
            ],
            out_specs=pl.BlockSpec((1, 256), lambda i, p: (0, 0)),
        ),
        compiler_params=pltpu.CompilerParams(vmem_limit_bytes=4 * 2**20),
        name="pauli",
    )(at, w_part, x, z)


def on_device(amplitudes, pauli_x, pauli_z, pauli_phase):
    total_cols = amplitudes.shape[1] * 128
    core = lax.axis_index(CORE)
    z_at = lax.axis_index(("gy_0", "gz_1"))
    pos = jnp.stack([lax.axis_index("gx"), lax.axis_index("gz_0"), z_at, core]).astype(jnp.int32)
    lt, w_own, w_other = prepare(pos, amplitudes)
    part = functools.partial(chunk_part, pos, lt)
    send1 = part(w_other, CHUNKS[0])
    recv1 = swapped(send1)
    send2 = part(w_other, CHUNKS[1], waits=(send1,))
    recv2 = swapped(send2)
    far0, far1 = part(w_own, CHUNKS[0], recv1, waits=(send2,))
    via_left = round_ring(far0, 0, 1)
    via_right = round_ring(far1, 0, -1)
    send3 = part(w_other, CHUNKS[2], waits=(far0,))
    recv3 = swapped(send3)
    right1, left0 = part(w_own, CHUNKS[1], recv2, waits=(send3,))
    from_left1 = round_ring(right1, 0, 1)
    from_right0 = round_ring(left0, 0, -1)
    send4 = part(w_other, CHUNKS[3], waits=(right1,))
    recv4 = swapped(send4)
    right0, left1 = part(w_own, CHUNKS[2], recv3, waits=(send4,))
    from_left0 = round_ring(right0 + via_left, 0, 1)
    from_right1 = round_ring(left1 + via_right, 0, -1)
    mine0, mine1 = part(w_own, CHUNKS[3], recv4, waits=(right0,))
    rows = []
    for mine, left, right in ((mine0, from_left0, from_right0), (mine1, from_left1, from_right1)):
        rows += [mine[k : k + 128] + left[k : k + 128] + right[k : k + 128] for k in (0, 128)]
    arrived = {k: round_ring(rows[k], 1, k) for k in (2, 1, 3)}
    rows = [
        sum((arrived[m][k : k + 32] for m in (1, 2, 3)), rows[0][k : k + 32]) for k in (0, 32, 64, 96)
    ]
    arrived = {k: round_ring(rows[k], 2, k) for k in (2, 1, 3)}
    both = (rows[0] + arrived[1] + arrived[2] + arrived[3]) * (1.0 / total_cols)
    first = lax.axis_index(AX) * 16
    first_rows = (first - core * 128).astype(jnp.int32)
    parts = pauli_parts(jnp.stack([first_rows, core.astype(jnp.int32)]), both, pauli_x[None], pauli_z[None])
    blocks = both.reshape(32, 64, 16).transpose(1, 2, 0).reshape(64, 512)
    message = jnp.concatenate([blocks, jnp.broadcast_to(parts, (64, 256))], 1).reshape(64, 6, 128)
    keep = lax.dynamic_slice_in_dim(both, core * 16, 16, 0)
    got = swapped(lax.dynamic_slice_in_dim(both, (1 - core) * 16, 16, 0))
    arrived = lax.all_to_all(message, SAME_CORE, split_axis=0, concat_axis=0, tiled=True)
    even_cols = jnp.where(core == 0, keep, got).reshape(16, 8, 128)
    odd_cols = jnp.where(core == 0, got, keep).reshape(16, 8, 128)
    w_rows = jnp.stack([even_cols, odd_cols], 2).reshape(16, 2048)
    sums = arrived[:, 4:].sum(0).reshape(256)[:200]
    sums = sums + swapped(sums)
    w_cols = arrived[:, :4].reshape(8, 8, 16, 2, 16).transpose(2, 0, 3, 1, 4).reshape(16, 2048)
    row = first + jnp.arange(16, dtype=jnp.int32)[:, None]
    col = jnp.arange(2048, dtype=jnp.int32)[None]
    density_real = jnp.where(col <= row, w_rows, w_cols)
    density_imag = jnp.where(col > row, w_rows, jnp.where(col < row, -w_cols, 0.0))
    even = parity_sign(pauli_x, pauli_z) > 0
    sum_real = jnp.where(even, sums, 0.0)
    sum_imag = jnp.where(even, 0.0, sums)
    phase_real, phase_imag = phase_parts(pauli_phase)
    expectations = jnp.stack(
        [phase_real * sum_real - phase_imag * sum_imag, phase_real * sum_imag + phase_imag * sum_real], 0
    )
    return density_real, density_imag, expectations


def solution(mesh):
    finer = Mesh(mesh.devices.reshape(mesh.shape["gx"], 2, 2, 4, 2), AX)
    in_specs = (P(None, AX, None), P(), P(), P())
    out_specs = (P(AX, None), P(AX, None), P())
    return jax.shard_map(on_device, mesh=finer, in_specs=in_specs, out_specs=out_specs, check_vma=False)
```

```python
import functools

import jax
import jax.numpy as jnp
from jax import lax
from jax.experimental import pallas as pl
from jax.experimental.pallas import tpu as pltpu
from jax.sharding import Mesh
from jax.sharding import PartitionSpec as P

AX = ("gx", "gy_0", "gy_1", "gz_0", "gz_1")
CORE = "gy_1"
SAME_CORE = ("gx", "gy_0", "gz_0", "gz_1")
CHUNK = 512


def device_index(x, y, z, core):
    return x * 32 + (z >> 1) * 16 + core * 8 + y * 2 + (z & 1)


def ring_perm(turn, step):
    pairs = []
    for x in range(4):
        for y in range(4):
            for z in range(4):
                for core in range(2):
                    to = [x, y, z]
                    axis = (turn + core) % 3
                    to[axis] = (to[axis] + step) % 4
                    pairs.append((device_index(x, y, z, core), device_index(*to, core)))
    return pairs


def round_ring(array, turn, step):
    return lax.ppermute(array, AX, ring_perm(turn, step))


def swapped(array):
    return lax.ppermute(array, CORE, [(0, 1), (1, 0)])


def prepare_kernel(pos_ref, a_ref, lt_ref, own_ref, other_ref):
    core = pos_ref[3]
    for block in range(16):
        cols = slice(block * 128, (block + 1) * 128)
        re = a_ref[0, :, cols].T
        im = a_ref[1, :, cols].T
        lt_ref[cols, 0:512] = re
        lt_ref[cols, 512:1024] = im
        lt_ref[cols, 1024:1536] = -re
    for block in range(8):
        cols = slice(block * 128, (block + 1) * 128)
        for ref, which in ((own_ref, core), (other_ref, core ^ 1)):
            from_cols = pl.ds(pl.multiple_of(block * 256 + which * 128, 128), 128)
            ref[:, cols] = a_ref[:, :, from_cols].reshape(1024, 128)


def prepare(pos, amps):
    return pl.pallas_call(
        prepare_kernel,
        out_shape=[
            jax.ShapeDtypeStruct((2048, 1536), jnp.bfloat16),
            jax.ShapeDtypeStruct((1024, 1024), jnp.bfloat16),
            jax.ShapeDtypeStruct((1024, 1024), jnp.bfloat16),
        ],
        grid_spec=pltpu.PrefetchScalarGridSpec(
            num_scalar_prefetch=1,
            grid=(1,),
            in_specs=[pl.BlockSpec((2, 512, 2048), lambda i, p: (0, 0, 0))],
            out_specs=[
                pl.BlockSpec((2048, 1536), lambda i, p: (0, 0)),
                pl.BlockSpec((1024, 1024), lambda i, p: (0, 0)),
                pl.BlockSpec((1024, 1024), lambda i, p: (0, 0)),
            ],
        ),
        compiler_params=pltpu.CompilerParams(vmem_limit_bytes=20 * 2**20),
        cost_estimate=pl.CostEstimate(flops=2 * 10**9, bytes_accessed=14 * 2**20, transcendentals=0),
        name="prepare",
    )(pos, amps)


CHUNKS = (((2, 0), (2, 1)), ((1, 1), (3, 0)), ((1, 0), (3, 1)), ((0, 0), (0, 1)))


def chunk_kernel(pos_ref, lt_ref, w_ref, *refs, halves, own, adds, waits):
    refs = refs[waits:]
    recv_ref = refs[0] if adds else None
    *outs, rows_ref, ids_ref = refs[1:] if adds else refs
    whose = pos_ref[3] if own else pos_ref[3] ^ 1
    lane = lax.broadcasted_iota(jnp.int32, (16, 128), 0)
    at = 0
    for k1, half in halves:
        for k2 in (2 * half, 2 * half + 1):
            for k3 in range(4):
                ahead = [(k1, k2, k3), (k3, k1, k2)]
                x, y, z = [
                    (pos_ref[n] + jnp.where(whose == 0, ahead[0][n], ahead[1][n])) & 3 for n in range(3)
                ]
                base = x * 512 + (z >> 1) * 256 + y * 32 + (z & 1) * 16
                for co in range(2):
                    row = pl.multiple_of(base + co * 128, 16)
                    rows_ref[at : at + 16, :] = lt_ref[pl.ds(row, 16), :]
                    ids_ref[at : at + 16, :] = lane + row
                    at += 16
    for tile in range(4):
        cols = slice(tile * 256, (tile + 1) * 256)
        real = jnp.dot(rows_ref[:, 0:1024], w_ref[:, cols], preferred_element_type=jnp.float32)
        imag = jnp.dot(rows_ref[:, 512:1536], w_ref[:, cols], preferred_element_type=jnp.float32)
        for part in range(2):
            here = slice(part * 128, (part + 1) * 128)
            to = slice(tile * 256 + part * 128, tile * 256 + (part + 1) * 128)
            col = lax.broadcasted_iota(jnp.int32, (CHUNK, 128), 1) + ((tile * 2 + part) * 256 + whose * 128)
            value = jnp.where(ids_ref[...] >= col, real[:, here], imag[:, here])
            if adds:
                value = value + recv_ref[:, to]
            if own:
                outs[0][:, to] = value[: CHUNK // 2]
                outs[1][:, to] = value[CHUNK // 2 :]
            else:
                outs[0][:, to] = value


def chunk_part(pos, lt, w, halves, own, recv=None, waits=()):
    adds = recv is not None
    full = pl.BlockSpec((CHUNK, 1024), lambda i, p: (0, 0))
    half = pl.BlockSpec((CHUNK // 2, 1024), lambda i, p: (0, 0))
    args = (pos, lt, w, *waits) + ((recv,) if adds else ())
    in_specs = [
        pl.BlockSpec((2048, 1536), lambda i, p: (0, 0)),
        pl.BlockSpec((1024, 1024), lambda i, p: (0, 0)),
        *[pl.BlockSpec(memory_space=pl.ANY) for _ in waits],
    ]
    if adds:
        in_specs.append(full)
    if own:
        out_shape = [jax.ShapeDtypeStruct((CHUNK // 2, 1024), jnp.float32)] * 2
    else:
        out_shape = jax.ShapeDtypeStruct((CHUNK, 1024), jnp.float32)
    return pl.pallas_call(
        functools.partial(chunk_kernel, halves=halves, own=own, adds=adds, waits=len(waits)),
        out_shape=out_shape,
        grid_spec=pltpu.PrefetchScalarGridSpec(
            num_scalar_prefetch=1,
            grid=(1,),
            in_specs=in_specs,
            out_specs=[half] * 2 if own else full,
            scratch_shapes=[pltpu.VMEM((CHUNK, 1536), jnp.bfloat16), pltpu.VMEM((CHUNK, 128), jnp.int32)],
        ),
        compiler_params=pltpu.CompilerParams(vmem_limit_bytes=12 * 2**20),
        cost_estimate=pl.CostEstimate(
            flops=4 * CHUNK * 1024 * 1024, bytes_accessed=2**20 * 8, transcendentals=0
        ),
        name="own" if own else "other",
    )(*args)


def parity_sign(values, masks):
    anded = jnp.bitwise_and(values, masks)
    for shift in (8, 4, 2, 1):
        anded = jnp.bitwise_xor(anded, jnp.right_shift(anded, shift))
    return (1 - 2 * jnp.bitwise_and(anded, 1)).astype(jnp.float32)


def phase_parts(pauli_phase):
    real = jnp.where(pauli_phase == 0, 1.0, jnp.where(pauli_phase == 2, -1.0, 0.0))
    imag = jnp.where(pauli_phase == 1, 1.0, jnp.where(pauli_phase == 3, -1.0, 0.0))
    return real.astype(jnp.float32), imag.astype(jnp.float32)


def pauli_kernel(at_ref, w_ref, x_ref, z_ref, out_ref):
    own = lax.broadcasted_iota(jnp.int32, (32, 128), 0)
    row = at_ref[0] + jnp.where(own >= 16, own + 112, own)
    for half in range(2):
        cols = slice(half * 128, (half + 1) * 128)
        x, z = x_ref[:, cols], z_ref[:, cols]
        col = jnp.bitwise_xor(row, x)
        lane = jnp.bitwise_and(col, 127)
        block = jnp.right_shift(col, 7)
        picked = jnp.zeros((32, 128), jnp.float32)
        for b in range(8):
            got = jnp.take_along_axis(w_ref[:, b * 128 : (b + 1) * 128], lane, axis=1)
            picked = jnp.where(block == 2 * b + at_ref[1], got, picked)
        found = jnp.where(col <= row, 1.0, -1.0)
        twice = jnp.where(x == 0, 1.0, 2.0)
        here = jnp.where(found == parity_sign(x, z), parity_sign(row, z) * picked, 0.0)
        out_ref[:, cols] = twice * jnp.sum(here, axis=0, keepdims=True)


def pauli_parts(at, w_part, x, z):
    return pl.pallas_call(
        pauli_kernel,
        out_shape=jax.ShapeDtypeStruct((1, 256), jnp.float32),
        grid_spec=pltpu.PrefetchScalarGridSpec(
            num_scalar_prefetch=1,
            grid=(1,),
            in_specs=[
                pl.BlockSpec((32, 1024), lambda i, p: (0, 0)),
                pl.BlockSpec((1, 256), lambda i, p: (0, 0)),
                pl.BlockSpec((1, 256), lambda i, p: (0, 0)),
            ],
            out_specs=pl.BlockSpec((1, 256), lambda i, p: (0, 0)),
        ),
        compiler_params=pltpu.CompilerParams(vmem_limit_bytes=4 * 2**20),
        name="pauli",
    )(at, w_part, x, z)


def swap_blocks(value):
    row = lax.broadcasted_iota(jnp.int32, (8, 128), 0)
    group = jnp.right_shift(lax.broadcasted_iota(jnp.int32, (8, 128), 1), 4)
    for step in (4, 2, 1):
        up = pltpu.roll(pltpu.roll(value, 8 - step, 0), 16 * step, 1)
        down = up if step == 4 else pltpu.roll(pltpu.roll(value, step, 0), 128 - 16 * step, 1)
        low_row = jnp.bitwise_and(row, step) == 0
        low_group = jnp.bitwise_and(group, step) == 0
        value = jnp.where(low_row, jnp.where(low_group, value, up), jnp.where(low_group, down, value))
    return value


def densities_kernel(place_ref, keep_ref, got_ref, col_ref, real_ref, imag_ref):
    first, core = place_ref[0], place_ref[1]
    row = lax.broadcasted_iota(jnp.int32, (8, 128), 0)
    lane = lax.broadcasted_iota(jnp.int32, (8, 128), 1)
    for t in range(8):
        for high in range(2):
            here = slice(high * 8, (high + 1) * 8)
            kept = keep_ref[here, t * 128 : (t + 1) * 128]
            got = got_ref[here, t * 128 : (t + 1) * 128]
            for co in range(2):
                across = swap_blocks(
                    col_ref[t * 8 : (t + 1) * 8, (co * 2 + high) * 128 : (co * 2 + high + 1) * 128]
                )
                mine = jnp.where(core == co, kept, got)
                i = row + (first + high * 8)
                j = lane + (t * 256 + co * 128)
                cols = slice(t * 256 + co * 128, t * 256 + (co + 1) * 128)
                real_ref[here, cols] = jnp.where(j <= i, mine, across)
                imag_ref[here, cols] = jnp.where(j > i, mine, jnp.where(j < i, -across, 0.0))


def densities(place, keep, got, arrived):
    rows = pl.BlockSpec((16, 1024), lambda i, p: (0, 0))
    out = pl.BlockSpec((16, 2048), lambda i, p: (0, 0))
    return pl.pallas_call(
        densities_kernel,
        out_shape=[jax.ShapeDtypeStruct((16, 2048), jnp.float32)] * 2,
        grid_spec=pltpu.PrefetchScalarGridSpec(
            num_scalar_prefetch=1,
            grid=(1,),
            in_specs=[rows, rows, pl.BlockSpec((64, 768), lambda i, p: (0, 0))],
            out_specs=[out, out],
        ),
        compiler_params=pltpu.CompilerParams(vmem_limit_bytes=4 * 2**20),
        name="densities",
    )(place, keep, got, arrived)


def on_device(amplitudes, pauli_x, pauli_z, pauli_phase):
    total_cols = amplitudes.shape[1] * 128
    core = lax.axis_index(CORE)
    z_at = lax.axis_index(("gy_0", "gz_1"))
    pos = jnp.stack([lax.axis_index("gx"), lax.axis_index("gz_0"), z_at, core]).astype(jnp.int32)
    lt, w_own, w_other = prepare(pos, amplitudes)
    send = functools.partial(chunk_part, pos, lt, w_other, own=False)
    make = functools.partial(chunk_part, pos, lt, w_own, own=True)
    send1 = send(CHUNKS[0])
    recv1 = swapped(send1)
    far0, far1 = make(CHUNKS[0], waits=(send1,))
    far0, far1 = far0 + recv1[: CHUNK // 2], far1 + recv1[CHUNK // 2 :]
    via_left = round_ring(far0, 0, 1)
    via_right = round_ring(far1, 0, -1)
    send2 = send(CHUNKS[1], waits=(far0,))
    recv2 = swapped(send2)
    send3 = send(CHUNKS[2], waits=(send2,))
    recv3 = swapped(send3)
    right1, left0 = make(CHUNKS[1], recv=recv2, waits=(send3,))
    from_left1 = round_ring(right1, 0, 1)
    from_right0 = round_ring(left0, 0, -1)
    send4 = send(CHUNKS[3], waits=(right1,))
    recv4 = swapped(send4)
    right0, left1 = make(CHUNKS[2], recv=recv3, waits=(send4,))
    from_left0 = round_ring(right0 + via_left, 0, 1)
    from_right1 = round_ring(left1 + via_right, 0, -1)
    mine0, mine1 = make(CHUNKS[3], recv=recv4, waits=(right0,))
    from_left0, from_left1, from_right0, from_right1 = lax.optimization_barrier(
        (from_left0, from_left1, from_right0, from_right1)
    )
    rows = []
    for mine, left, right in ((mine0, from_left0, from_right0), (mine1, from_left1, from_right1)):
        rows += [mine[k : k + 128] + left[k : k + 128] + right[k : k + 128] for k in (0, 128)]
    arrived = {}
    for k in (2, 1, 3):
        arrived[k] = round_ring(rows[k], 1, k)
    rows = [
        sum((arrived[m][k : k + 32] for m in (1, 2, 3)), rows[0][k : k + 32]) for k in (0, 32, 64, 96)
    ]
    arrived = {}
    for k in (2, 1, 3):
        arrived[k] = round_ring(rows[k], 2, k)
    both = (rows[0] + arrived[1] + arrived[2] + arrived[3]) * (1.0 / total_cols)
    first = lax.axis_index(AX) * 16
    first_rows = (first - core * 128).astype(jnp.int32)
    parts = pauli_parts(jnp.stack([first_rows, core.astype(jnp.int32)]), both, pauli_x[None], pauli_z[None])
    blocks = both.reshape(2, 16, 64, 16).transpose(2, 0, 3, 1).reshape(64, 512)
    message = jnp.concatenate([blocks, jnp.broadcast_to(parts, (64, 256))], 1)
    keep = lax.dynamic_slice_in_dim(both, core * 16, 16, 0)
    got = swapped(lax.dynamic_slice_in_dim(both, (1 - core) * 16, 16, 0))
    arrived = lax.all_to_all(message, SAME_CORE, split_axis=0, concat_axis=0, tiled=True)
    sums = arrived[:, 512:].sum(0)[:200]
    sums = sums + swapped(sums)
    place = jnp.stack([first.astype(jnp.int32), core.astype(jnp.int32)])
    density_real, density_imag = densities(place, keep, got, arrived)
    even = parity_sign(pauli_x, pauli_z) > 0
    sum_real = jnp.where(even, sums, 0.0)
    sum_imag = jnp.where(even, 0.0, sums)
    phase_real, phase_imag = phase_parts(pauli_phase)
    expectations = jnp.stack(
        [phase_real * sum_real - phase_imag * sum_imag, phase_real * sum_imag + phase_imag * sum_real], 0
    )
    return density_real, density_imag, expectations


def solution(mesh):
    finer = Mesh(mesh.devices.reshape(mesh.shape["gx"], 2, 2, 4, 2), AX)
    in_specs = (P(None, AX, None), P(), P(), P())
    out_specs = (P(AX, None), P(AX, None), P())
    return jax.shard_map(on_device, mesh=finer, in_specs=in_specs, out_specs=out_specs, check_vma=False)
```

```python
import functools

import jax
import jax.numpy as jnp
from jax import lax
from jax.experimental import pallas as pl
from jax.experimental.pallas import tpu as pltpu
from jax.sharding import Mesh
from jax.sharding import PartitionSpec as P

AX = ("gx", "gy_0", "gy_1", "gz_0", "gz_1")
CORE = "gy_1"
SAME_CORE = ("gx", "gy_0", "gz_0", "gz_1")
CHUNK = 512


def device_index(x, y, z, core):
    return x * 32 + (z >> 1) * 16 + core * 8 + y * 2 + (z & 1)


def ring_perm(turn, step):
    pairs = []
    for x in range(4):
        for y in range(4):
            for z in range(4):
                for core in range(2):
                    to = [x, y, z]
                    axis = (turn + core) % 3
                    to[axis] = (to[axis] + step) % 4
                    pairs.append((device_index(x, y, z, core), device_index(*to, core)))
    return pairs


def round_ring(array, turn, step):
    return lax.ppermute(array, AX, ring_perm(turn, step))


def swapped(array):
    return lax.ppermute(array, CORE, [(0, 1), (1, 0)])


def prepare_kernel(pos_ref, a_ref, lt_ref, own_ref, other_ref):
    core = pos_ref[3]
    for block in range(16):
        cols = slice(block * 128, (block + 1) * 128)
        re = a_ref[0, :, cols].T
        im = a_ref[1, :, cols].T
        lt_ref[cols, 0:512] = re
        lt_ref[cols, 512:1024] = im
        lt_ref[cols, 1024:1536] = -re
    for block in range(8):
        cols = slice(block * 128, (block + 1) * 128)
        for ref, which in ((own_ref, core), (other_ref, core ^ 1)):
            from_cols = pl.ds(pl.multiple_of(block * 256 + which * 128, 128), 128)
            ref[:, cols] = a_ref[:, :, from_cols].reshape(1024, 128)


def prepare(pos, amps):
    return pl.pallas_call(
        prepare_kernel,
        out_shape=[
            jax.ShapeDtypeStruct((2048, 1536), jnp.bfloat16),
            jax.ShapeDtypeStruct((1024, 1024), jnp.bfloat16),
            jax.ShapeDtypeStruct((1024, 1024), jnp.bfloat16),
        ],
        grid_spec=pltpu.PrefetchScalarGridSpec(
            num_scalar_prefetch=1,
            grid=(1,),
            in_specs=[pl.BlockSpec((2, 512, 2048), lambda i, p: (0, 0, 0))],
            out_specs=[
                pl.BlockSpec((2048, 1536), lambda i, p: (0, 0)),
                pl.BlockSpec((1024, 1024), lambda i, p: (0, 0)),
                pl.BlockSpec((1024, 1024), lambda i, p: (0, 0)),
            ],
        ),
        compiler_params=pltpu.CompilerParams(vmem_limit_bytes=20 * 2**20),
        cost_estimate=pl.CostEstimate(flops=2 * 10**9, bytes_accessed=14 * 2**20, transcendentals=0),
        name="prepare",
    )(pos, amps)


CHUNKS = (((2, 0), (2, 1)), ((1, 1), (3, 0)), ((1, 0), (3, 1)), ((0, 0), (0, 1)))


def chunk_kernel(pos_ref, lt_ref, w_ref, *refs, halves, own, waits):
    *outs, rows_ref, ids_ref = refs[waits:]
    whose = pos_ref[3] if own else pos_ref[3] ^ 1
    lane = lax.broadcasted_iota(jnp.int32, (16, 128), 0)
    at = 0
    for k1, half in halves:
        for k2 in (2 * half, 2 * half + 1):
            for k3 in range(4):
                ahead = [(k1, k2, k3), (k3, k1, k2)]
                x, y, z = [
                    (pos_ref[n] + jnp.where(whose == 0, ahead[0][n], ahead[1][n])) & 3 for n in range(3)
                ]
                base = x * 512 + (z >> 1) * 256 + y * 32 + (z & 1) * 16
                for co in range(2):
                    row = pl.multiple_of(base + co * 128, 16)
                    rows_ref[at : at + 16, :] = lt_ref[pl.ds(row, 16), :]
                    ids_ref[at : at + 16, :] = lane + row
                    at += 16
    for tile in range(4):
        cols = slice(tile * 256, (tile + 1) * 256)
        real = jnp.dot(rows_ref[:, 0:1024], w_ref[:, cols], preferred_element_type=jnp.float32)
        imag = jnp.dot(rows_ref[:, 512:1536], w_ref[:, cols], preferred_element_type=jnp.float32)
        for part in range(2):
            here = slice(part * 128, (part + 1) * 128)
            to = slice(tile * 256 + part * 128, tile * 256 + (part + 1) * 128)
            col = lax.broadcasted_iota(jnp.int32, (CHUNK, 128), 1) + ((tile * 2 + part) * 256 + whose * 128)
            value = jnp.where(ids_ref[...] >= col, real[:, here], imag[:, here])
            if own:
                outs[0][:, to] = value[: CHUNK // 2]
                outs[1][:, to] = value[CHUNK // 2 :]
            else:
                outs[0][:, to] = value


def chunk_part(pos, lt, w, halves, own, waits=()):
    full = pl.BlockSpec((CHUNK, 1024), lambda i, p: (0, 0))
    half = pl.BlockSpec((CHUNK // 2, 1024), lambda i, p: (0, 0))
    args = (pos, lt, w, *waits)
    in_specs = [
        pl.BlockSpec((2048, 1536), lambda i, p: (0, 0)),
        pl.BlockSpec((1024, 1024), lambda i, p: (0, 0)),
        *[pl.BlockSpec(memory_space=pl.ANY) for _ in waits],
    ]
    if own:
        out_shape = [jax.ShapeDtypeStruct((CHUNK // 2, 1024), jnp.float32)] * 2
    else:
        out_shape = jax.ShapeDtypeStruct((CHUNK, 1024), jnp.float32)
    return pl.pallas_call(
        functools.partial(chunk_kernel, halves=halves, own=own, waits=len(waits)),
        out_shape=out_shape,
        grid_spec=pltpu.PrefetchScalarGridSpec(
            num_scalar_prefetch=1,
            grid=(1,),
            in_specs=in_specs,
            out_specs=[half] * 2 if own else full,
            scratch_shapes=[pltpu.VMEM((CHUNK, 1536), jnp.bfloat16), pltpu.VMEM((CHUNK, 128), jnp.int32)],
        ),
        compiler_params=pltpu.CompilerParams(vmem_limit_bytes=12 * 2**20),
        cost_estimate=pl.CostEstimate(
            flops=4 * CHUNK * 1024 * 1024, bytes_accessed=2**20 * 8, transcendentals=0
        ),
        name="own" if own else "other",
    )(*args)


def parity_sign(values, masks):
    anded = jnp.bitwise_and(values, masks)
    for shift in (8, 4, 2, 1):
        anded = jnp.bitwise_xor(anded, jnp.right_shift(anded, shift))
    return (1 - 2 * jnp.bitwise_and(anded, 1)).astype(jnp.float32)


def phase_parts(pauli_phase):
    real = jnp.where(pauli_phase == 0, 1.0, jnp.where(pauli_phase == 2, -1.0, 0.0))
    imag = jnp.where(pauli_phase == 1, 1.0, jnp.where(pauli_phase == 3, -1.0, 0.0))
    return real.astype(jnp.float32), imag.astype(jnp.float32)


def pauli_kernel(at_ref, w_ref, x_ref, z_ref, out_ref):
    own = lax.broadcasted_iota(jnp.int32, (32, 128), 0)
    row = at_ref[0] + jnp.where(own >= 16, own + 112, own)
    for half in range(2):
        cols = slice(half * 128, (half + 1) * 128)
        x, z = x_ref[:, cols], z_ref[:, cols]
        col = jnp.bitwise_xor(row, x)
        lane = jnp.bitwise_and(col, 127)
        block = jnp.right_shift(col, 7)
        picked = jnp.zeros((32, 128), jnp.float32)
        for b in range(8):
            got = jnp.take_along_axis(w_ref[:, b * 128 : (b + 1) * 128], lane, axis=1)
            picked = jnp.where(block == 2 * b + at_ref[1], got, picked)
        found = jnp.where(col <= row, 1.0, -1.0)
        twice = jnp.where(x == 0, 1.0, 2.0)
        here = jnp.where(found == parity_sign(x, z), parity_sign(row, z) * picked, 0.0)
        out_ref[:, cols] = twice * jnp.sum(here, axis=0, keepdims=True)


def pauli_parts(at, w_part, x, z):
    return pl.pallas_call(
        pauli_kernel,
        out_shape=jax.ShapeDtypeStruct((1, 256), jnp.float32),
        grid_spec=pltpu.PrefetchScalarGridSpec(
            num_scalar_prefetch=1,
            grid=(1,),
            in_specs=[
                pl.BlockSpec((32, 1024), lambda i, p: (0, 0)),
                pl.BlockSpec((1, 256), lambda i, p: (0, 0)),
                pl.BlockSpec((1, 256), lambda i, p: (0, 0)),
            ],
            out_specs=pl.BlockSpec((1, 256), lambda i, p: (0, 0)),
        ),
        compiler_params=pltpu.CompilerParams(vmem_limit_bytes=4 * 2**20),
        name="pauli",
    )(at, w_part, x, z)


def swap_blocks(value):
    row = lax.broadcasted_iota(jnp.int32, (8, 128), 0)
    group = jnp.right_shift(lax.broadcasted_iota(jnp.int32, (8, 128), 1), 4)
    for step in (4, 2, 1):
        up = pltpu.roll(pltpu.roll(value, 8 - step, 0), 16 * step, 1)
        down = up if step == 4 else pltpu.roll(pltpu.roll(value, step, 0), 128 - 16 * step, 1)
        low_row = jnp.bitwise_and(row, step) == 0
        low_group = jnp.bitwise_and(group, step) == 0
        value = jnp.where(low_row, jnp.where(low_group, value, up), jnp.where(low_group, down, value))
    return value


def densities_kernel(place_ref, keep_ref, got_ref, col_ref, real_ref, imag_ref):
    first, core = place_ref[0], place_ref[1]
    row = lax.broadcasted_iota(jnp.int32, (8, 128), 0)
    lane = lax.broadcasted_iota(jnp.int32, (8, 128), 1)
    for t in range(8):
        for high in range(2):
            here = slice(high * 8, (high + 1) * 8)
            kept = keep_ref[here, t * 128 : (t + 1) * 128]
            got = got_ref[here, t * 128 : (t + 1) * 128]
            for co in range(2):
                across = swap_blocks(
                    col_ref[t * 8 : (t + 1) * 8, (co * 2 + high) * 128 : (co * 2 + high + 1) * 128]
                )
                mine = jnp.where(core == co, kept, got)
                i = row + (first + high * 8)
                j = lane + (t * 256 + co * 128)
                cols = slice(t * 256 + co * 128, t * 256 + (co + 1) * 128)
                real_ref[here, cols] = jnp.where(j <= i, mine, across)
                imag_ref[here, cols] = jnp.where(j > i, mine, jnp.where(j < i, -across, 0.0))


def densities(place, keep, got, arrived):
    rows = pl.BlockSpec((16, 1024), lambda i, p: (0, 0))
    out = pl.BlockSpec((16, 2048), lambda i, p: (0, 0))
    return pl.pallas_call(
        densities_kernel,
        out_shape=[jax.ShapeDtypeStruct((16, 2048), jnp.float32)] * 2,
        grid_spec=pltpu.PrefetchScalarGridSpec(
            num_scalar_prefetch=1,
            grid=(1,),
            in_specs=[rows, rows, pl.BlockSpec((64, 768), lambda i, p: (0, 0))],
            out_specs=[out, out],
        ),
        compiler_params=pltpu.CompilerParams(vmem_limit_bytes=4 * 2**20),
        name="densities",
    )(place, keep, got, arrived)


def on_device(amplitudes, pauli_x, pauli_z, pauli_phase):
    total_cols = amplitudes.shape[1] * 128
    core = lax.axis_index(CORE)
    z_at = lax.axis_index(("gy_0", "gz_1"))
    pos = jnp.stack([lax.axis_index("gx"), lax.axis_index("gz_0"), z_at, core]).astype(jnp.int32)
    lt, w_own, w_other = prepare(pos, amplitudes)
    send = functools.partial(chunk_part, pos, lt, w_other, own=False)
    make = functools.partial(chunk_part, pos, lt, w_own, own=True)
    send1 = send(CHUNKS[0])
    recv1 = swapped(send1)
    far = make(CHUNKS[0], waits=(send1,))
    far0, far1 = far[0] + recv1[:256], far[1] + recv1[256:]
    via_left = round_ring(far0, 0, 1)
    via_right = round_ring(far1, 0, -1)
    send2 = send(CHUNKS[1], waits=(far0,))
    recv2 = swapped(send2)
    near = make(CHUNKS[1], waits=(send2,))
    right1, left0 = near[0] + recv2[:256], near[1] + recv2[256:]
    from_left1 = round_ring(right1, 0, 1)
    from_right0 = round_ring(left0, 0, -1)
    send3 = send(CHUNKS[2], waits=(near[0],))
    recv3 = swapped(send3)
    near = make(CHUNKS[2], waits=(send3,))
    from_left0 = round_ring(near[0] + recv3[:256] + via_left, 0, 1)
    from_right1 = round_ring(near[1] + recv3[256:] + via_right, 0, -1)
    send4 = send(CHUNKS[3], waits=(near[0],))
    recv4 = swapped(send4)
    mine = make(CHUNKS[3], waits=(send4,))
    came = lax.optimization_barrier(((from_left0, from_right0), (from_left1, from_right1)))

    def first_sum(came, half, at):
        left, right = came[half]
        here = slice(at, at + 64)
        return (mine[half][here] + recv4[half * 256 + at : half * 256 + at + 64]) + (left[here] + right[here])

    places = ((1, 0), (1, 64), (0, 192), (1, 128))
    (far0, far1, right1, left0), came = lax.optimization_barrier(
        (tuple(first_sum(came, *p) for p in places), came)
    )
    via_left = round_ring(far0, 1, 1)
    via_right = round_ring(far1, 1, -1)
    from_left1 = round_ring(right1, 1, 1)
    from_right0 = round_ring(left0, 1, -1)
    places = ((0, 128), (1, 192), (0, 0), (0, 64))
    right0, left1, low, high = lax.optimization_barrier(tuple(first_sum(came, *p) for p in places))
    from_left0 = round_ring(right0 + via_left, 1, 1)
    from_right1 = round_ring(left1 + via_right, 1, -1)
    low = low + from_left0 + from_right0
    high = high + from_left1 + from_right1
    rows = [low[:32], low[32:], high[:32], high[32:]]
    arrived = {}
    for k in (2, 1, 3):
        arrived[k] = round_ring(rows[k], 2, k)
    both = (rows[0] + arrived[1] + arrived[2] + arrived[3]) * (1.0 / total_cols)
    first = lax.axis_index(AX) * 16
    first_rows = (first - core * 128).astype(jnp.int32)
    parts = pauli_parts(jnp.stack([first_rows, core.astype(jnp.int32)]), both, pauli_x[None], pauli_z[None])
    blocks = both.reshape(2, 16, 64, 16).transpose(2, 0, 3, 1).reshape(64, 512)
    message = jnp.concatenate([blocks, jnp.broadcast_to(parts, (64, 256))], 1)
    keep = lax.dynamic_slice_in_dim(both, core * 16, 16, 0)
    got = swapped(lax.dynamic_slice_in_dim(both, (1 - core) * 16, 16, 0))
    arrived = lax.all_to_all(message, SAME_CORE, split_axis=0, concat_axis=0, tiled=True)
    sums = arrived[:, 512:].sum(0)[:200]
    sums = sums + swapped(sums)
    place = jnp.stack([first.astype(jnp.int32), core.astype(jnp.int32)])
    density_real, density_imag = densities(place, keep, got, arrived)
    even = parity_sign(pauli_x, pauli_z) > 0
    sum_real = jnp.where(even, sums, 0.0)
    sum_imag = jnp.where(even, 0.0, sums)
    phase_real, phase_imag = phase_parts(pauli_phase)
    expectations = jnp.stack(
        [phase_real * sum_real - phase_imag * sum_imag, phase_real * sum_imag + phase_imag * sum_real], 0
    )
    return density_real, density_imag, expectations


def solution(mesh):
    finer = Mesh(mesh.devices.reshape(mesh.shape["gx"], 2, 2, 4, 2), AX)
    in_specs = (P(None, AX, None), P(), P(), P())
    out_specs = (P(AX, None), P(AX, None), P())
    return jax.shard_map(on_device, mesh=finer, in_specs=in_specs, out_specs=out_specs, check_vma=False)
```

```python
import functools

import jax
import jax.numpy as jnp
from jax import lax
from jax.experimental import pallas as pl
from jax.experimental.pallas import tpu as pltpu
from jax.sharding import Mesh
from jax.sharding import PartitionSpec as P

AX = ("gx", "gy_0", "gy_1", "gz_0", "gz_1")
CORE = "gy_1"
SAME_CORE = ("gx", "gy_0", "gz_0", "gz_1")
CHUNK = 512


def device_index(x, y, z, core):
    return x * 32 + (z >> 1) * 16 + core * 8 + y * 2 + (z & 1)


def ring_perm(turn, step):
    pairs = []
    for x in range(4):
        for y in range(4):
            for z in range(4):
                for core in range(2):
                    to = [x, y, z]
                    axis = (turn + 1 + core) % 3
                    to[axis] = (to[axis] + step) % 4
                    pairs.append((device_index(x, y, z, core), device_index(*to, core)))
    return pairs


def round_ring(array, turn, step):
    return lax.ppermute(array, AX, ring_perm(turn, step))


def swapped(array):
    return lax.ppermute(array, CORE, [(0, 1), (1, 0)])


STEPS = 8


def prepare_kernel(pos_ref, amps_ref, lt_ref, own_ref, other_ref, a_ref, sems):
    core = pos_ref[3]
    width = 2048 // STEPS
    copies = []
    for step in range(STEPS):
        cols = slice(step * width, (step + 1) * width)
        copy = pltpu.make_async_copy(amps_ref.at[:, :, cols], a_ref.at[:, :, cols], sems.at[step])
        copy.start()
        copies.append(copy)
    for step in range(STEPS):
        copies[step].wait()
        for block in range(step * width // 128, (step + 1) * width // 128):
            cols = slice(block * 128, (block + 1) * 128)
            re = a_ref[0, :, cols].T
            im = a_ref[1, :, cols].T
            lt_ref[cols, 0:512] = re
            lt_ref[cols, 512:1024] = im
            lt_ref[cols, 1024:1536] = -re
        for block in range(step * width // 256, (step + 1) * width // 256):
            cols = slice(block * 128, (block + 1) * 128)
            for ref, which in ((own_ref, core), (other_ref, core ^ 1)):
                from_cols = pl.ds(pl.multiple_of(block * 256 + which * 128, 128), 128)
                ref[:, cols] = a_ref[:, :, from_cols].reshape(1024, 128)


def prepare(pos, amps):
    return pl.pallas_call(
        prepare_kernel,
        out_shape=[
            jax.ShapeDtypeStruct((2048, 1536), jnp.bfloat16),
            jax.ShapeDtypeStruct((1024, 1024), jnp.bfloat16),
            jax.ShapeDtypeStruct((1024, 1024), jnp.bfloat16),
        ],
        grid_spec=pltpu.PrefetchScalarGridSpec(
            num_scalar_prefetch=1,
            grid=(1,),
            in_specs=[pl.BlockSpec(memory_space=pltpu.HBM)],
            out_specs=[
                pl.BlockSpec((2048, 1536), lambda i, p: (0, 0)),
                pl.BlockSpec((1024, 1024), lambda i, p: (0, 0)),
                pl.BlockSpec((1024, 1024), lambda i, p: (0, 0)),
            ],
            scratch_shapes=[pltpu.VMEM((2, 512, 2048), jnp.bfloat16), pltpu.SemaphoreType.DMA((STEPS,))],
        ),
        compiler_params=pltpu.CompilerParams(vmem_limit_bytes=26 * 2**20),
        cost_estimate=pl.CostEstimate(flops=2 * 10**9, bytes_accessed=14 * 2**20, transcendentals=0),
        name="prepare",
    )(pos, pltpu.with_memory_space_constraint(amps, pltpu.HBM))


CHUNKS = (((2, 0), (2, 1)), ((1, 1), (3, 0)), ((1, 0), (3, 1)), ((0, 0), (0, 1)))


def chunk_kernel(pos_ref, lt_ref, w_ref, *refs, halves, own, waits):
    out_ref, rows_ref, ids_ref = refs[waits:]
    whose = pos_ref[3] if own else pos_ref[3] ^ 1
    first = whose == 0
    x0, y0, z0 = pos_ref[0], pos_ref[1], pos_ref[2]
    lane = lax.broadcasted_iota(jnp.int32, (16, 128), 0)
    col = lax.broadcasted_iota(jnp.int32, (1, 256), 1)
    col = jnp.where(col >= 128, col + 128, col) + whose * 128
    to = []
    for x in range(4):
        kx = (x - x0) & 3
        pick = (kx >> 1) ^ halves[0][1]
        k1_there = jnp.where(pick == 0, halves[0][0], halves[1][0])
        for s in range(4):
            h, j = divmod(s, 2)
            k1, half = halves[h]
            y = jnp.where(first, (y0 + k1) & 3, s)
            z = jnp.where(first, z0 + 2 * half + j, z0 + k1_there) & 3
            here = h * 256 + j * 128 + kx * 32
            there = pick * 256 + (kx & 1) * 128 + ((s - y0) & 3) * 32
            to.append(pl.multiple_of(jnp.where(first, here, there), 32))
            base = x * 512 + (z >> 1) * 256 + y * 32 + (z & 1) * 16
            for co in range(2):
                at = x * 128 + s * 32 + co * 16
                row = pl.multiple_of(base + co * 128, 16)
                rows_ref[at : at + 16, :] = lt_ref[pl.ds(row, 16), :]
                ids_ref[at : at + 16, :] = lane + row
    for tile in range(4):
        cols = slice(tile * 256, (tile + 1) * 256)
        w = w_ref[:, cols]
        real = jnp.dot(rows_ref[tile * 128 :, 0:1024], w, preferred_element_type=jnp.float32)
        imag = jnp.dot(rows_ref[: (tile + 1) * 128, 512:1536], w, preferred_element_type=jnp.float32)
        for x in range(4):
            if x > tile:
                value = real[(x - tile) * 128 : (x - tile + 1) * 128]
            elif x < tile:
                value = imag[x * 128 : (x + 1) * 128]
            else:
                ids = ids_ref[x * 128 : (x + 1) * 128, :]
                lower = jnp.concatenate([ids, ids], 1) >= col + tile * 512
                value = jnp.where(lower, real[:128], imag[x * 128 :])
            for s in range(4):
                out_ref[pl.ds(to[x * 4 + s], 32), cols] = value[s * 32 : (s + 1) * 32]


def chunk_part(pos, lt, w, halves, own, waits=()):
    full = pl.BlockSpec((CHUNK, 1024), lambda i, p: (0, 0))
    return pl.pallas_call(
        functools.partial(chunk_kernel, halves=halves, own=own, waits=len(waits)),
        out_shape=jax.ShapeDtypeStruct((CHUNK, 1024), jnp.float32),
        grid_spec=pltpu.PrefetchScalarGridSpec(
            num_scalar_prefetch=1,
            grid=(1,),
            in_specs=[
                pl.BlockSpec((2048, 1536), lambda i, p: (0, 0)),
                pl.BlockSpec((1024, 1024), lambda i, p: (0, 0)),
                *[pl.BlockSpec(memory_space=pl.ANY) for _ in waits],
            ],
            out_specs=full,
            scratch_shapes=[pltpu.VMEM((CHUNK, 1536), jnp.bfloat16), pltpu.VMEM((CHUNK, 128), jnp.int32)],
        ),
        compiler_params=pltpu.CompilerParams(vmem_limit_bytes=12 * 2**20),
        cost_estimate=pl.CostEstimate(
            flops=5 * CHUNK * 512 * 1024, bytes_accessed=2**20 * 8, transcendentals=0
        ),
        name="own" if own else "other",
    )(pos, lt, w, *waits)


def parity_sign(values, masks):
    anded = jnp.bitwise_and(values, masks)
    for shift in (8, 4, 2, 1):
        anded = jnp.bitwise_xor(anded, jnp.right_shift(anded, shift))
    return (1 - 2 * jnp.bitwise_and(anded, 1)).astype(jnp.float32)


def phase_parts(pauli_phase):
    real = jnp.where(pauli_phase == 0, 1.0, jnp.where(pauli_phase == 2, -1.0, 0.0))
    imag = jnp.where(pauli_phase == 1, 1.0, jnp.where(pauli_phase == 3, -1.0, 0.0))
    return real.astype(jnp.float32), imag.astype(jnp.float32)


def pauli_kernel(at_ref, w_ref, x_ref, z_ref, out_ref):
    own = lax.broadcasted_iota(jnp.int32, (32, 128), 0)
    row = at_ref[0] + jnp.where(own >= 16, own + 112, own)
    for half in range(2):
        cols = slice(half * 128, (half + 1) * 128)
        x, z = x_ref[:, cols], z_ref[:, cols]
        col = jnp.bitwise_xor(row, x)
        lane = jnp.bitwise_and(col, 127)
        block = jnp.right_shift(col, 7)
        picked = jnp.zeros((32, 128), jnp.float32)
        for b in range(8):
            got = jnp.take_along_axis(w_ref[:, b * 128 : (b + 1) * 128], lane, axis=1)
            picked = jnp.where(block == 2 * b + at_ref[1], got, picked)
        found = jnp.where(col <= row, 1.0, -1.0)
        twice = jnp.where(x == 0, 1.0, 2.0)
        here = jnp.where(found == parity_sign(x, z), parity_sign(row, z) * picked, 0.0)
        out_ref[:, cols] = twice * jnp.sum(here, axis=0, keepdims=True)


def pauli_parts(at, w_part, x, z):
    return pl.pallas_call(
        pauli_kernel,
        out_shape=jax.ShapeDtypeStruct((1, 256), jnp.float32),
        grid_spec=pltpu.PrefetchScalarGridSpec(
            num_scalar_prefetch=1,
            grid=(1,),
            in_specs=[
                pl.BlockSpec((32, 1024), lambda i, p: (0, 0)),
                pl.BlockSpec((1, 256), lambda i, p: (0, 0)),
                pl.BlockSpec((1, 256), lambda i, p: (0, 0)),
            ],
            out_specs=pl.BlockSpec((1, 256), lambda i, p: (0, 0)),
        ),
        compiler_params=pltpu.CompilerParams(vmem_limit_bytes=4 * 2**20),
        name="pauli",
    )(at, w_part, x, z)


def swap_blocks(value):
    row = lax.broadcasted_iota(jnp.int32, (8, 128), 0)
    group = jnp.right_shift(lax.broadcasted_iota(jnp.int32, (8, 128), 1), 4)
    for step in (4, 2, 1):
        up = pltpu.roll(pltpu.roll(value, 8 - step, 0), 16 * step, 1)
        down = up if step == 4 else pltpu.roll(pltpu.roll(value, step, 0), 128 - 16 * step, 1)
        low_row = jnp.bitwise_and(row, step) == 0
        low_group = jnp.bitwise_and(group, step) == 0
        value = jnp.where(low_row, jnp.where(low_group, value, up), jnp.where(low_group, down, value))
    return value


def densities_kernel(place_ref, keep_ref, got_ref, col_ref, real_ref, imag_ref):
    first, core = place_ref[0], place_ref[1]
    row = lax.broadcasted_iota(jnp.int32, (8, 128), 0)
    lane = lax.broadcasted_iota(jnp.int32, (8, 128), 1)
    for t in range(8):
        for high in range(2):
            here = slice(high * 8, (high + 1) * 8)
            kept = keep_ref[here, t * 128 : (t + 1) * 128]
            got = got_ref[here, t * 128 : (t + 1) * 128]
            for co in range(2):
                across = swap_blocks(
                    col_ref[t * 8 : (t + 1) * 8, (co * 2 + high) * 128 : (co * 2 + high + 1) * 128]
                )
                mine = jnp.where(core == co, kept, got)
                i = row + (first + high * 8)
                j = lane + (t * 256 + co * 128)
                cols = slice(t * 256 + co * 128, t * 256 + (co + 1) * 128)
                real_ref[here, cols] = jnp.where(j <= i, mine, across)
                imag_ref[here, cols] = jnp.where(j > i, mine, jnp.where(j < i, -across, 0.0))


def densities(place, keep, got, arrived):
    rows = pl.BlockSpec((16, 1024), lambda i, p: (0, 0))
    out = pl.BlockSpec((16, 2048), lambda i, p: (0, 0))
    return pl.pallas_call(
        densities_kernel,
        out_shape=[jax.ShapeDtypeStruct((16, 2048), jnp.float32)] * 2,
        grid_spec=pltpu.PrefetchScalarGridSpec(
            num_scalar_prefetch=1,
            grid=(1,),
            in_specs=[rows, rows, pl.BlockSpec((64, 768), lambda i, p: (0, 0))],
            out_specs=[out, out],
        ),
        compiler_params=pltpu.CompilerParams(vmem_limit_bytes=4 * 2**20),
        name="densities",
    )(place, keep, got, arrived)


def on_device(amplitudes, pauli_x, pauli_z, pauli_phase):
    total_cols = amplitudes.shape[1] * 128
    core = lax.axis_index(CORE)
    z_at = lax.axis_index(("gy_0", "gz_1"))
    pos = jnp.stack([lax.axis_index("gx"), lax.axis_index("gz_0"), z_at, core]).astype(jnp.int32)
    lt, w_own, w_other = prepare(pos, amplitudes)
    send = functools.partial(chunk_part, pos, lt, w_other, own=False)
    make = functools.partial(chunk_part, pos, lt, w_own, own=True)
    send1 = send(CHUNKS[0])
    recv1 = swapped(send1)
    far = make(CHUNKS[0], waits=(send1,))
    far0, far1 = far[:256] + recv1[:256], far[256:] + recv1[256:]
    via_left = round_ring(far0, 0, 1)
    via_right = round_ring(far1, 0, -1)
    send2 = send(CHUNKS[1], waits=(far0,))
    recv2 = swapped(send2)
    near = make(CHUNKS[1], waits=(send2,))
    right1, left0 = near[:256] + recv2[:256], near[256:] + recv2[256:]
    from_left1 = round_ring(right1, 0, 1)
    from_right0 = round_ring(left0, 0, -1)
    send3 = send(CHUNKS[2], waits=(near,))
    recv3 = swapped(send3)
    near = make(CHUNKS[2], waits=(send3,))
    from_left0 = round_ring(near[:256] + recv3[:256] + via_left, 0, 1)
    from_right1 = round_ring(near[256:] + recv3[256:] + via_right, 0, -1)
    send4 = send(CHUNKS[3], waits=(near,))
    recv4 = swapped(send4)
    mine = make(CHUNKS[3], waits=(send4,))
    came = lax.optimization_barrier(((from_left0, from_right0), (from_left1, from_right1)))

    def first_sum(came, half, at):
        left, right = came[half]
        here = slice(at, at + 64)
        there = slice(half * 256 + at, half * 256 + at + 64)
        return (mine[there] + recv4[there]) + (left[here] + right[here])

    places = ((1, 0), (1, 64), (0, 192), (1, 128))
    (far0, far1, right1, left0), came = lax.optimization_barrier(
        (tuple(first_sum(came, *p) for p in places), came)
    )
    via_left = round_ring(far0, 1, 1)
    via_right = round_ring(far1, 1, -1)
    from_left1 = round_ring(right1, 1, 1)
    from_right0 = round_ring(left0, 1, -1)
    places = ((0, 128), (1, 192), (0, 0), (0, 64))
    right0, left1, low, high = lax.optimization_barrier(tuple(first_sum(came, *p) for p in places))
    from_left0 = round_ring(right0 + via_left, 1, 1)
    from_right1 = round_ring(left1 + via_right, 1, -1)
    low = low + from_left0 + from_right0
    high = high + from_left1 + from_right1
    rows = [low[:32], low[32:], high[:32], high[32:]]
    arrived = {}
    for k in (2, 1, 3):
        arrived[k] = round_ring(rows[k], 2, k)
    both = (rows[0] + arrived[1] + arrived[2] + arrived[3]) * (1.0 / total_cols)
    first = lax.axis_index(AX) * 16
    first_rows = (first - core * 128).astype(jnp.int32)
    parts = pauli_parts(jnp.stack([first_rows, core.astype(jnp.int32)]), both, pauli_x[None], pauli_z[None])
    blocks = both.reshape(2, 16, 64, 16).transpose(2, 0, 3, 1).reshape(64, 512)
    message = jnp.concatenate([blocks, jnp.broadcast_to(parts, (64, 256))], 1)
    keep = lax.dynamic_slice_in_dim(both, core * 16, 16, 0)
    got = swapped(lax.dynamic_slice_in_dim(both, (1 - core) * 16, 16, 0))
    arrived = lax.all_to_all(message, SAME_CORE, split_axis=0, concat_axis=0, tiled=True)
    sums = arrived[:, 512:].sum(0)[:200]
    sums = sums + swapped(sums)
    place = jnp.stack([first.astype(jnp.int32), core.astype(jnp.int32)])
    density_real, density_imag = densities(place, keep, got, arrived)
    even = parity_sign(pauli_x, pauli_z) > 0
    sum_real = jnp.where(even, sums, 0.0)
    sum_imag = jnp.where(even, 0.0, sums)
    phase_real, phase_imag = phase_parts(pauli_phase)
    expectations = jnp.stack(
        [phase_real * sum_real - phase_imag * sum_imag, phase_real * sum_imag + phase_imag * sum_real], 0
    )
    return density_real, density_imag, expectations


def solution(mesh):
    finer = Mesh(mesh.devices.reshape(mesh.shape["gx"], 2, 2, 4, 2), AX)
    in_specs = (P(None, AX, None), P(), P(), P())
    out_specs = (P(AX, None), P(AX, None), P())
    return jax.shard_map(on_device, mesh=finer, in_specs=in_specs, out_specs=out_specs, check_vma=False)
```

```python
import functools

import jax
import jax.numpy as jnp
from jax import lax
from jax.experimental import pallas as pl
from jax.experimental.pallas import tpu as pltpu
from jax.sharding import Mesh
from jax.sharding import PartitionSpec as P

AX = ("gx", "gy_0", "gy_1", "gz_0", "gz_1")
CORE = "gy_1"
SAME_CORE = ("gx", "gy_0", "gz_0", "gz_1")
CHUNK = 512


def device_index(x, y, z, core):
    return x * 32 + (z >> 1) * 16 + core * 8 + y * 2 + (z & 1)


def ring_perm(turn, step):
    pairs = []
    for x in range(4):
        for y in range(4):
            for z in range(4):
                for core in range(2):
                    to = [x, y, z]
                    axis = (turn + 1 + core) % 3
                    to[axis] = (to[axis] + step) % 4
                    pairs.append((device_index(x, y, z, core), device_index(*to, core)))
    return pairs


def round_ring(array, turn, step):
    return lax.ppermute(array, AX, ring_perm(turn, step))


def swapped(array):
    return lax.ppermute(array, CORE, [(0, 1), (1, 0)])


STEPS = 8


def prepare_kernel(pos_ref, amps_ref, lt_ref, own_ref, other_ref, a_ref, sems):
    core = pos_ref[3]
    width = 2048 // STEPS
    copies = []
    for step in range(STEPS):
        cols = slice(step * width, (step + 1) * width)
        copy = pltpu.make_async_copy(amps_ref.at[:, :, cols], a_ref.at[:, :, cols], sems.at[step])
        copy.start()
        copies.append(copy)
    for step in range(STEPS):
        copies[step].wait()
        for block in range(step * width // 128, (step + 1) * width // 128):
            cols = slice(block * 128, (block + 1) * 128)
            re = a_ref[0, :, cols].T
            im = a_ref[1, :, cols].T
            lt_ref[cols, 0:512] = re
            lt_ref[cols, 512:1024] = im
            lt_ref[cols, 1024:1536] = -re
        for block in range(step * width // 256, (step + 1) * width // 256):
            cols = slice(block * 128, (block + 1) * 128)
            for ref, which in ((own_ref, core), (other_ref, core ^ 1)):
                from_cols = pl.ds(pl.multiple_of(block * 256 + which * 128, 128), 128)
                ref[:, cols] = a_ref[:, :, from_cols].reshape(1024, 128)


def prepare(pos, amps):
    return pl.pallas_call(
        prepare_kernel,
        out_shape=[
            jax.ShapeDtypeStruct((2048, 1536), jnp.bfloat16),
            jax.ShapeDtypeStruct((1024, 1024), jnp.bfloat16),
            jax.ShapeDtypeStruct((1024, 1024), jnp.bfloat16),
        ],
        grid_spec=pltpu.PrefetchScalarGridSpec(
            num_scalar_prefetch=1,
            grid=(1,),
            in_specs=[pl.BlockSpec(memory_space=pltpu.HBM)],
            out_specs=[
                pl.BlockSpec((2048, 1536), lambda i, p: (0, 0)),
                pl.BlockSpec((1024, 1024), lambda i, p: (0, 0)),
                pl.BlockSpec((1024, 1024), lambda i, p: (0, 0)),
            ],
            scratch_shapes=[pltpu.VMEM((2, 512, 2048), jnp.bfloat16), pltpu.SemaphoreType.DMA((STEPS,))],
        ),
        compiler_params=pltpu.CompilerParams(vmem_limit_bytes=26 * 2**20),
        cost_estimate=pl.CostEstimate(flops=2 * 10**9, bytes_accessed=14 * 2**20, transcendentals=0),
        name="prepare",
    )(pos, pltpu.with_memory_space_constraint(amps, pltpu.HBM))


SECOND = ((2, 1), (3, 0))
CHUNKS = (((2, 0), (2, 1)), ((1, 1), (3, 0)), ((1, 0), (3, 1)), ((0, 0), (0, 1)))


def chunk_kernel(pos_ref, lt_ref, w_ref, *refs, halves, own, waits):
    out_ref, rows_ref, ids_ref = refs[waits:]
    whose = pos_ref[3] if own else pos_ref[3] ^ 1
    first = whose == 0
    x0, y0, z0 = pos_ref[0], pos_ref[1], pos_ref[2]
    lane = lax.broadcasted_iota(jnp.int32, (16, 128), 0)
    col = lax.broadcasted_iota(jnp.int32, (1, 256), 1)
    col = jnp.where(col >= 128, col + 128, col) + whose * 128
    to = []
    for x in range(4):
        kx = (x - x0) & 3
        pick = (((kx ^ (kx >> 1)) & 1) ^ 1) ^ halves[0][1]
        k1_there = jnp.where(pick == 0, halves[0][0], halves[1][0])
        for s in range(4):
            h, j = divmod(s, 2)
            k1, half = halves[h]
            y = jnp.where(first, (y0 + k1) & 3, s)
            z = jnp.where(first, z0 + SECOND[half][j], z0 + k1_there) & 3
            here = h * 256 + j * 128 + kx * 32
            there = pick * 256 + (1 - (kx >> 1)) * 128 + ((s - y0) & 3) * 32
            to.append(pl.multiple_of(jnp.where(first, here, there), 32))
            base = x * 512 + (z >> 1) * 256 + y * 32 + (z & 1) * 16
            for co in range(2):
                at = x * 128 + s * 32 + co * 16
                row = pl.multiple_of(base + co * 128, 16)
                rows_ref[at : at + 16, :] = lt_ref[pl.ds(row, 16), :]
                ids_ref[at : at + 16, :] = lane + row
    for tile in range(4):
        cols = slice(tile * 256, (tile + 1) * 256)
        w = w_ref[:, cols]
        real = jnp.dot(rows_ref[tile * 128 :, 0:1024], w, preferred_element_type=jnp.float32)
        imag = jnp.dot(rows_ref[: (tile + 1) * 128, 512:1536], w, preferred_element_type=jnp.float32)
        for x in range(4):
            if x > tile:
                value = real[(x - tile) * 128 : (x - tile + 1) * 128]
            elif x < tile:
                value = imag[x * 128 : (x + 1) * 128]
            else:
                ids = ids_ref[x * 128 : (x + 1) * 128, :]
                lower = jnp.concatenate([ids, ids], 1) >= col + tile * 512
                value = jnp.where(lower, real[:128], imag[x * 128 :])
            for s in range(4):
                out_ref[pl.ds(to[x * 4 + s], 32), cols] = value[s * 32 : (s + 1) * 32]


def chunk_part(pos, lt, w, halves, own, waits=()):
    full = pl.BlockSpec((CHUNK, 1024), lambda i, p: (0, 0))
    return pl.pallas_call(
        functools.partial(chunk_kernel, halves=halves, own=own, waits=len(waits)),
        out_shape=jax.ShapeDtypeStruct((CHUNK, 1024), jnp.float32),
        grid_spec=pltpu.PrefetchScalarGridSpec(
            num_scalar_prefetch=1,
            grid=(1,),
            in_specs=[
                pl.BlockSpec((2048, 1536), lambda i, p: (0, 0)),
                pl.BlockSpec((1024, 1024), lambda i, p: (0, 0)),
                *[pl.BlockSpec(memory_space=pl.ANY) for _ in waits],
            ],
            out_specs=full,
            scratch_shapes=[pltpu.VMEM((CHUNK, 1536), jnp.bfloat16), pltpu.VMEM((CHUNK, 128), jnp.int32)],
        ),
        compiler_params=pltpu.CompilerParams(vmem_limit_bytes=12 * 2**20),
        cost_estimate=pl.CostEstimate(
            flops=5 * CHUNK * 512 * 1024, bytes_accessed=2**20 * 8, transcendentals=0
        ),
        name="own" if own else "other",
    )(pos, lt, w, *waits)


def parity_sign(values, masks):
    anded = jnp.bitwise_and(values, masks)
    for shift in (8, 4, 2, 1):
        anded = jnp.bitwise_xor(anded, jnp.right_shift(anded, shift))
    return (1 - 2 * jnp.bitwise_and(anded, 1)).astype(jnp.float32)


def phase_parts(pauli_phase):
    real = jnp.where(pauli_phase == 0, 1.0, jnp.where(pauli_phase == 2, -1.0, 0.0))
    imag = jnp.where(pauli_phase == 1, 1.0, jnp.where(pauli_phase == 3, -1.0, 0.0))
    return real.astype(jnp.float32), imag.astype(jnp.float32)


def pauli_kernel(at_ref, w_ref, x_ref, z_ref, out_ref):
    own = lax.broadcasted_iota(jnp.int32, (32, 128), 0)
    row = at_ref[0] + jnp.where(own >= 16, own + 112, own)
    for half in range(2):
        cols = slice(half * 128, (half + 1) * 128)
        x, z = x_ref[:, cols], z_ref[:, cols]
        col = jnp.bitwise_xor(row, x)
        lane = jnp.bitwise_and(col, 127)
        block = jnp.right_shift(col, 7)
        picked = jnp.zeros((32, 128), jnp.float32)
        for b in range(8):
            got = jnp.take_along_axis(w_ref[:, b * 128 : (b + 1) * 128], lane, axis=1)
            picked = jnp.where(block == 2 * b + at_ref[1], got, picked)
        found = jnp.where(col <= row, 1.0, -1.0)
        twice = jnp.where(x == 0, 1.0, 2.0)
        here = jnp.where(found == parity_sign(x, z), parity_sign(row, z) * picked, 0.0)
        out_ref[:, cols] = twice * jnp.sum(here, axis=0, keepdims=True)


def pauli_parts(at, w_part, x, z):
    return pl.pallas_call(
        pauli_kernel,
        out_shape=jax.ShapeDtypeStruct((1, 256), jnp.float32),
        grid_spec=pltpu.PrefetchScalarGridSpec(
            num_scalar_prefetch=1,
            grid=(1,),
            in_specs=[
                pl.BlockSpec((32, 1024), lambda i, p: (0, 0)),
                pl.BlockSpec((1, 256), lambda i, p: (0, 0)),
                pl.BlockSpec((1, 256), lambda i, p: (0, 0)),
            ],
            out_specs=pl.BlockSpec((1, 256), lambda i, p: (0, 0)),
        ),
        compiler_params=pltpu.CompilerParams(vmem_limit_bytes=4 * 2**20),
        name="pauli",
    )(at, w_part, x, z)


def swap_blocks(value):
    row = lax.broadcasted_iota(jnp.int32, (8, 128), 0)
    group = jnp.right_shift(lax.broadcasted_iota(jnp.int32, (8, 128), 1), 4)
    for step in (4, 2, 1):
        up = pltpu.roll(pltpu.roll(value, 8 - step, 0), 16 * step, 1)
        down = up if step == 4 else pltpu.roll(pltpu.roll(value, step, 0), 128 - 16 * step, 1)
        low_row = jnp.bitwise_and(row, step) == 0
        low_group = jnp.bitwise_and(group, step) == 0
        value = jnp.where(low_row, jnp.where(low_group, value, up), jnp.where(low_group, down, value))
    return value


def densities_kernel(place_ref, keep_ref, got_ref, col_ref, real_ref, imag_ref):
    first, core = place_ref[0], place_ref[1]
    row = lax.broadcasted_iota(jnp.int32, (8, 128), 0)
    lane = lax.broadcasted_iota(jnp.int32, (8, 128), 1)
    for t in range(8):
        for high in range(2):
            here = slice(high * 8, (high + 1) * 8)
            kept = keep_ref[here, t * 128 : (t + 1) * 128]
            got = got_ref[here, t * 128 : (t + 1) * 128]
            for co in range(2):
                across = swap_blocks(
                    col_ref[t * 8 : (t + 1) * 8, (co * 2 + high) * 128 : (co * 2 + high + 1) * 128]
                )
                mine = jnp.where(core == co, kept, got)
                i = row + (first + high * 8)
                j = lane + (t * 256 + co * 128)
                cols = slice(t * 256 + co * 128, t * 256 + (co + 1) * 128)
                real_ref[here, cols] = jnp.where(j <= i, mine, across)
                imag_ref[here, cols] = jnp.where(j > i, mine, jnp.where(j < i, -across, 0.0))


def densities(place, keep, got, arrived):
    rows = pl.BlockSpec((16, 1024), lambda i, p: (0, 0))
    out = pl.BlockSpec((16, 2048), lambda i, p: (0, 0))
    return pl.pallas_call(
        densities_kernel,
        out_shape=[jax.ShapeDtypeStruct((16, 2048), jnp.float32)] * 2,
        grid_spec=pltpu.PrefetchScalarGridSpec(
            num_scalar_prefetch=1,
            grid=(1,),
            in_specs=[rows, rows, pl.BlockSpec((64, 768), lambda i, p: (0, 0))],
            out_specs=[out, out],
        ),
        compiler_params=pltpu.CompilerParams(vmem_limit_bytes=4 * 2**20),
        name="densities",
    )(place, keep, got, arrived)


def on_device(amplitudes, pauli_x, pauli_z, pauli_phase):
    total_cols = amplitudes.shape[1] * 128
    core = lax.axis_index(CORE)
    z_at = lax.axis_index(("gy_0", "gz_1"))
    pos = jnp.stack([lax.axis_index("gx"), lax.axis_index("gz_0"), z_at, core]).astype(jnp.int32)
    lt, w_own, w_other = prepare(pos, amplitudes)
    send = functools.partial(chunk_part, pos, lt, w_other, own=False)
    make = functools.partial(chunk_part, pos, lt, w_own, own=True)
    send1 = send(CHUNKS[0])
    recv1 = swapped(send1)
    far = make(CHUNKS[0], waits=(send1,))
    far0, far1 = far[:256] + recv1[:256], far[256:] + recv1[256:]
    via_left = round_ring(far0, 0, 1)
    via_right = round_ring(far1, 0, -1)
    send2 = send(CHUNKS[1], waits=(far0,))
    recv2 = swapped(send2)
    near = make(CHUNKS[1], waits=(send2,))
    right1, left0 = near[:256] + recv2[:256], near[256:] + recv2[256:]
    from_left1 = round_ring(right1, 0, 1)
    from_right0 = round_ring(left0, 0, -1)
    send3 = send(CHUNKS[2], waits=(near,))
    recv3 = swapped(send3)
    near = make(CHUNKS[2], waits=(send3,))
    from_left0 = round_ring(near[:256] + recv3[:256] + via_left, 0, 1)
    from_right1 = round_ring(near[256:] + recv3[256:] + via_right, 0, -1)
    send4 = send(CHUNKS[3], waits=(near,))
    recv4 = swapped(send4)
    mine = make(CHUNKS[3], waits=(send4,))
    def first_sum(came, half, at):
        left, right = came
        here = slice(at, at + 64)
        there = slice(half * 256 + at, half * 256 + at + 64)
        return (mine[there] + recv4[there]) + (left[here] + right[here])

    came = lax.optimization_barrier((from_left0, from_right0))
    sums = tuple(first_sum(came, 0, at) for at in (0, 64, 128, 192))
    far0, far1, right0, right1 = lax.optimization_barrier(sums)
    via_left = round_ring(far0, 1, 1)
    via_right = round_ring(far1, 1, -1)
    next_left1 = round_ring(right1, 1, 1)
    came = lax.optimization_barrier((from_left1, from_right1))
    left0, left1, low, high = lax.optimization_barrier(tuple(first_sum(came, 1, at) for at in (0, 64, 128, 192)))
    next_right0 = round_ring(left0, 1, -1)
    next_left0 = round_ring(right0 + via_left, 1, 1)
    next_right1 = round_ring(left1 + via_right, 1, -1)
    low = low + next_left0 + next_right0
    high = high + next_left1 + next_right1
    rows = [low[:32], low[32:], high[:32], high[32:]]
    arrived = {}
    for k in (2, 1, 3):
        arrived[k] = round_ring(rows[k], 2, k)
    both = (rows[0] + arrived[1] + arrived[2] + arrived[3]) * (1.0 / total_cols)
    first = lax.axis_index(AX) * 16
    first_rows = (first - core * 128).astype(jnp.int32)
    parts = pauli_parts(jnp.stack([first_rows, core.astype(jnp.int32)]), both, pauli_x[None], pauli_z[None])
    blocks = both.reshape(2, 16, 64, 16).transpose(2, 0, 3, 1).reshape(64, 512)
    message = jnp.concatenate([blocks, jnp.broadcast_to(parts, (64, 256))], 1)
    keep = lax.dynamic_slice_in_dim(both, core * 16, 16, 0)
    got = swapped(lax.dynamic_slice_in_dim(both, (1 - core) * 16, 16, 0))
    arrived = lax.all_to_all(message, SAME_CORE, split_axis=0, concat_axis=0, tiled=True)
    sums = arrived[:, 512:].sum(0)[:200]
    sums = sums + swapped(sums)
    place = jnp.stack([first.astype(jnp.int32), core.astype(jnp.int32)])
    density_real, density_imag = densities(place, keep, got, arrived)
    even = parity_sign(pauli_x, pauli_z) > 0
    sum_real = jnp.where(even, sums, 0.0)
    sum_imag = jnp.where(even, 0.0, sums)
    phase_real, phase_imag = phase_parts(pauli_phase)
    expectations = jnp.stack(
        [phase_real * sum_real - phase_imag * sum_imag, phase_real * sum_imag + phase_imag * sum_real], 0
    )
    return density_real, density_imag, expectations


def solution(mesh):
    finer = Mesh(mesh.devices.reshape(mesh.shape["gx"], 2, 2, 4, 2), AX)
    in_specs = (P(None, AX, None), P(), P(), P())
    out_specs = (P(AX, None), P(AX, None), P())
    return jax.shard_map(on_device, mesh=finer, in_specs=in_specs, out_specs=out_specs, check_vma=False)
```

```python
import functools

import jax
import jax.numpy as jnp
from jax import lax
from jax.experimental import pallas as pl
from jax.experimental.pallas import tpu as pltpu
from jax.sharding import Mesh
from jax.sharding import PartitionSpec as P

AX = ("gx", "gy_0", "gy_1", "gz_0", "gz_1")
CORE = "gy_1"
SAME_CORE = ("gx", "gy_0", "gz_0", "gz_1")
CHUNK = 512


def device_index(x, y, z, core):
    return x * 32 + (z >> 1) * 16 + core * 8 + y * 2 + (z & 1)


def ring_perm(turn, step):
    pairs = []
    for x in range(4):
        for y in range(4):
            for z in range(4):
                for core in range(2):
                    to = [x, y, z]
                    axis = (turn + 1 + core) % 3
                    to[axis] = (to[axis] + step) % 4
                    pairs.append((device_index(x, y, z, core), device_index(*to, core)))
    return pairs


def round_ring(array, turn, step):
    return lax.ppermute(array, AX, ring_perm(turn, step))


def swapped(array):
    return lax.ppermute(array, CORE, [(0, 1), (1, 0)])


STEPS = 8


def prepare_kernel(pos_ref, amps_ref, lt_ref, own_ref, other_ref, a_ref, sems):
    core = pos_ref[3]
    width = 2048 // STEPS
    copies = []
    for step in range(STEPS):
        cols = slice(step * width, (step + 1) * width)
        copy = pltpu.make_async_copy(amps_ref.at[:, :, cols], a_ref.at[:, :, cols], sems.at[step])
        copy.start()
        copies.append(copy)
    for step in range(STEPS):
        copies[step].wait()
        for block in range(step * width // 128, (step + 1) * width // 128):
            cols = slice(block * 128, (block + 1) * 128)
            re = a_ref[0, :, cols].T
            im = a_ref[1, :, cols].T
            lt_ref[cols, 0:512] = re
            lt_ref[cols, 512:1024] = im
            lt_ref[cols, 1024:1536] = -re
        for block in range(step * width // 256, (step + 1) * width // 256):
            cols = slice(block * 128, (block + 1) * 128)
            for ref, which in ((own_ref, core), (other_ref, core ^ 1)):
                from_cols = pl.ds(pl.multiple_of(block * 256 + which * 128, 128), 128)
                ref[:, cols] = a_ref[:, :, from_cols].reshape(1024, 128)


def prepare(pos, amps):
    return pl.pallas_call(
        prepare_kernel,
        out_shape=[
            jax.ShapeDtypeStruct((2048, 1536), jnp.bfloat16),
            jax.ShapeDtypeStruct((1024, 1024), jnp.bfloat16),
            jax.ShapeDtypeStruct((1024, 1024), jnp.bfloat16),
        ],
        grid_spec=pltpu.PrefetchScalarGridSpec(
            num_scalar_prefetch=1,
            grid=(1,),
            in_specs=[pl.BlockSpec(memory_space=pltpu.HBM)],
            out_specs=[
                pl.BlockSpec((2048, 1536), lambda i, p: (0, 0)),
                pl.BlockSpec((1024, 1024), lambda i, p: (0, 0)),
                pl.BlockSpec((1024, 1024), lambda i, p: (0, 0)),
            ],
            scratch_shapes=[pltpu.VMEM((2, 512, 2048), jnp.bfloat16), pltpu.SemaphoreType.DMA((STEPS,))],
        ),
        compiler_params=pltpu.CompilerParams(vmem_limit_bytes=26 * 2**20),
        cost_estimate=pl.CostEstimate(flops=2 * 10**9, bytes_accessed=14 * 2**20, transcendentals=0),
        name="prepare",
    )(pos, pltpu.with_memory_space_constraint(amps, pltpu.HBM))


SECOND = ((2, 1), (3, 0))
CHUNKS = (((2, 0), (2, 1)), ((1, 1), (3, 0)), ((1, 0), (3, 1)), ((0, 0), (0, 1)))


def chunk_kernel(pos_ref, lt_ref, w_ref, *refs, halves, own, waits):
    out_ref, rows_ref, ids_ref = refs[waits:]
    whose = pos_ref[3] if own else pos_ref[3] ^ 1
    first = whose == 0
    x0, y0, z0 = pos_ref[0], pos_ref[1], pos_ref[2]
    lane = lax.broadcasted_iota(jnp.int32, (16, 128), 0)
    col = lax.broadcasted_iota(jnp.int32, (1, 256), 1)
    col = jnp.where(col >= 128, col + 128, col) + whose * 128
    to = []
    for x in range(4):
        kx = (x - x0) & 3
        pick = (((kx ^ (kx >> 1)) & 1) ^ 1) ^ halves[0][1]
        k1_there = jnp.where(pick == 0, halves[0][0], halves[1][0])
        for s in range(4):
            h, j = divmod(s, 2)
            k1, half = halves[h]
            y = jnp.where(first, (y0 + k1) & 3, s)
            z = jnp.where(first, z0 + SECOND[half][j], z0 + k1_there) & 3
            here = h * 256 + j * 128 + kx * 32
            there = pick * 256 + (1 - (kx >> 1)) * 128 + ((s - y0) & 3) * 32
            to.append(pl.multiple_of(jnp.where(first, here, there), 32))
            base = x * 512 + (z >> 1) * 256 + y * 32 + (z & 1) * 16
            for co in range(2):
                at = x * 128 + s * 32 + co * 16
                row = pl.multiple_of(base + co * 128, 16)
                rows_ref[at : at + 16, :] = lt_ref[pl.ds(row, 16), :]
                ids_ref[at : at + 16, :] = lane + row
    for tile in range(4):
        cols = slice(tile * 256, (tile + 1) * 256)
        w = w_ref[:, cols]
        real = jnp.dot(rows_ref[tile * 128 :, 0:1024], w, preferred_element_type=jnp.float32)
        imag = jnp.dot(rows_ref[: (tile + 1) * 128, 512:1536], w, preferred_element_type=jnp.float32)
        for x in range(4):
            if x > tile:
                value = real[(x - tile) * 128 : (x - tile + 1) * 128]
            elif x < tile:
                value = imag[x * 128 : (x + 1) * 128]
            else:
                ids = ids_ref[x * 128 : (x + 1) * 128, :]
                lower = jnp.concatenate([ids, ids], 1) >= col + tile * 512
                value = jnp.where(lower, real[:128], imag[x * 128 :])
            for s in range(4):
                out_ref[pl.ds(to[x * 4 + s], 32), cols] = value[s * 32 : (s + 1) * 32]


def chunk_part(pos, lt, w, halves, own, waits=()):
    full = pl.BlockSpec((CHUNK, 1024), lambda i, p: (0, 0))
    return pl.pallas_call(
        functools.partial(chunk_kernel, halves=halves, own=own, waits=len(waits)),
        out_shape=jax.ShapeDtypeStruct((CHUNK, 1024), jnp.float32),
        grid_spec=pltpu.PrefetchScalarGridSpec(
            num_scalar_prefetch=1,
            grid=(1,),
            in_specs=[
                pl.BlockSpec((2048, 1536), lambda i, p: (0, 0)),
                pl.BlockSpec((1024, 1024), lambda i, p: (0, 0)),
                *[pl.BlockSpec(memory_space=pl.ANY) for _ in waits],
            ],
            out_specs=full,
            scratch_shapes=[pltpu.VMEM((CHUNK, 1536), jnp.bfloat16), pltpu.VMEM((CHUNK, 128), jnp.int32)],
        ),
        compiler_params=pltpu.CompilerParams(vmem_limit_bytes=12 * 2**20),
        cost_estimate=pl.CostEstimate(
            flops=5 * CHUNK * 512 * 1024, bytes_accessed=2**20 * 8, transcendentals=0
        ),
        name="own" if own else "other",
    )(pos, lt, w, *waits)


def parity_sign(values, masks):
    anded = jnp.bitwise_and(values, masks)
    for shift in (8, 4, 2, 1):
        anded = jnp.bitwise_xor(anded, jnp.right_shift(anded, shift))
    return (1 - 2 * jnp.bitwise_and(anded, 1)).astype(jnp.float32)


def phase_parts(pauli_phase):
    real = jnp.where(pauli_phase == 0, 1.0, jnp.where(pauli_phase == 2, -1.0, 0.0))
    imag = jnp.where(pauli_phase == 1, 1.0, jnp.where(pauli_phase == 3, -1.0, 0.0))
    return real.astype(jnp.float32), imag.astype(jnp.float32)


def pauli_kernel(at_ref, w_ref, x_ref, z_ref, out_ref):
    own = lax.broadcasted_iota(jnp.int32, (32, 128), 0)
    row = at_ref[0] + jnp.where(own >= 16, own + 112, own)
    for half in range(2):
        cols = slice(half * 128, (half + 1) * 128)
        x, z = x_ref[:, cols], z_ref[:, cols]
        col = jnp.bitwise_xor(row, x)
        lane = jnp.bitwise_and(col, 127)
        block = jnp.right_shift(col, 7)
        picked = jnp.zeros((32, 128), jnp.float32)
        for b in range(8):
            got = jnp.take_along_axis(w_ref[:, b * 128 : (b + 1) * 128], lane, axis=1)
            picked = jnp.where(block == 2 * b + at_ref[1], got, picked)
        found = jnp.where(col <= row, 1.0, -1.0)
        twice = jnp.where(x == 0, 1.0, 2.0)
        here = jnp.where(found == parity_sign(x, z), parity_sign(row, z) * picked, 0.0)
        out_ref[:, cols] = twice * jnp.sum(here, axis=0, keepdims=True)


def pauli_parts(at, w_part, x, z):
    return pl.pallas_call(
        pauli_kernel,
        out_shape=jax.ShapeDtypeStruct((1, 256), jnp.float32),
        grid_spec=pltpu.PrefetchScalarGridSpec(
            num_scalar_prefetch=1,
            grid=(1,),
            in_specs=[
                pl.BlockSpec((32, 1024), lambda i, p: (0, 0)),
                pl.BlockSpec((1, 256), lambda i, p: (0, 0)),
                pl.BlockSpec((1, 256), lambda i, p: (0, 0)),
            ],
            out_specs=pl.BlockSpec((1, 256), lambda i, p: (0, 0)),
        ),
        compiler_params=pltpu.CompilerParams(vmem_limit_bytes=4 * 2**20),
        name="pauli",
    )(at, w_part, x, z)


def swap_blocks(value):
    row = lax.broadcasted_iota(jnp.int32, (8, 128), 0)
    group = jnp.right_shift(lax.broadcasted_iota(jnp.int32, (8, 128), 1), 4)
    for step in (4, 2, 1):
        up = pltpu.roll(pltpu.roll(value, 8 - step, 0), 16 * step, 1)
        down = up if step == 4 else pltpu.roll(pltpu.roll(value, step, 0), 128 - 16 * step, 1)
        low_row = jnp.bitwise_and(row, step) == 0
        low_group = jnp.bitwise_and(group, step) == 0
        value = jnp.where(low_row, jnp.where(low_group, value, up), jnp.where(low_group, down, value))
    return value


def densities_kernel(place_ref, keep_ref, got_ref, col_ref, x_ref, z_ref, phase_ref, real_ref, imag_ref, out_ref):
    sums = jnp.sum(col_ref[:, 512:], axis=0, keepdims=True)
    even = parity_sign(x_ref[...], z_ref[...]) > 0
    sum_real = jnp.where(even, sums, 0.0)
    sum_imag = jnp.where(even, 0.0, sums)
    phase_real, phase_imag = phase_parts(phase_ref[...])
    out_ref[0:1, :] = (phase_real * sum_real - phase_imag * sum_imag)[:, : out_ref.shape[1]]
    out_ref[1:2, :] = (phase_real * sum_imag + phase_imag * sum_real)[:, : out_ref.shape[1]]
    first, core = place_ref[0], place_ref[1]
    row = lax.broadcasted_iota(jnp.int32, (8, 128), 0)
    lane = lax.broadcasted_iota(jnp.int32, (8, 128), 1)
    for t in range(8):
        for high in range(2):
            here = slice(high * 8, (high + 1) * 8)
            kept = keep_ref[here, t * 128 : (t + 1) * 128]
            got = got_ref[here, t * 128 : (t + 1) * 128]
            for co in range(2):
                across = swap_blocks(
                    col_ref[t * 8 : (t + 1) * 8, (co * 2 + high) * 128 : (co * 2 + high + 1) * 128]
                )
                mine = jnp.where(core == co, kept, got)
                i = row + (first + high * 8)
                j = lane + (t * 256 + co * 128)
                cols = slice(t * 256 + co * 128, t * 256 + (co + 1) * 128)
                real_ref[here, cols] = jnp.where(j <= i, mine, across)
                imag_ref[here, cols] = jnp.where(j > i, mine, jnp.where(j < i, -across, 0.0))


def densities(place, keep, got, arrived, x, z, phase):
    terms = pl.BlockSpec((1, 256), lambda i, p: (0, 0))
    sums = (2, x.shape[1])
    rows = pl.BlockSpec((16, 1024), lambda i, p: (0, 0))
    out = pl.BlockSpec((16, 2048), lambda i, p: (0, 0))
    return pl.pallas_call(
        densities_kernel,
        out_shape=[jax.ShapeDtypeStruct((16, 2048), jnp.float32)] * 2 + [jax.ShapeDtypeStruct(sums, jnp.float32)],
        grid_spec=pltpu.PrefetchScalarGridSpec(
            num_scalar_prefetch=1,
            grid=(1,),
            in_specs=[rows, rows, pl.BlockSpec((64, 768), lambda i, p: (0, 0)), terms, terms, terms],
            out_specs=[out, out, pl.BlockSpec(sums, lambda i, p: (0, 0))],
        ),
        compiler_params=pltpu.CompilerParams(vmem_limit_bytes=4 * 2**20),
        name="densities",
    )(place, keep, got, arrived, x, z, phase)


def on_device(amplitudes, pauli_x, pauli_z, pauli_phase):
    total_cols = amplitudes.shape[1] * 128
    core = lax.axis_index(CORE)
    z_at = lax.axis_index(("gy_0", "gz_1"))
    pos = jnp.stack([lax.axis_index("gx"), lax.axis_index("gz_0"), z_at, core]).astype(jnp.int32)
    lt, w_own, w_other = prepare(pos, amplitudes)
    send = functools.partial(chunk_part, pos, lt, w_other, own=False)
    make = functools.partial(chunk_part, pos, lt, w_own, own=True)
    send1 = send(CHUNKS[0])
    recv1 = swapped(send1)
    far = make(CHUNKS[0], waits=(send1,))
    far0, far = lax.optimization_barrier((far[:256] + recv1[:256], far))
    far1 = far[256:] + recv1[256:]
    via_left = round_ring(far0, 0, 1)
    via_right = round_ring(far1, 0, -1)
    send2 = send(CHUNKS[1], waits=(far0,))
    recv2 = swapped(send2)
    near = make(CHUNKS[1], waits=(send2,))
    right1, left0 = near[:256] + recv2[:256], near[256:] + recv2[256:]
    from_left1 = round_ring(right1, 0, 1)
    from_right0 = round_ring(left0, 0, -1)
    send3 = send(CHUNKS[2], waits=(near,))
    recv3 = swapped(send3)
    near = make(CHUNKS[2], waits=(send3,))
    from_left0 = round_ring(near[:256] + recv3[:256] + via_left, 0, 1)
    from_right1 = round_ring(near[256:] + recv3[256:] + via_right, 0, -1)
    send4 = send(CHUNKS[3], waits=(near,))
    recv4 = swapped(send4)
    mine = make(CHUNKS[3], waits=(send4,))
    def first_sum(came, half, at):
        left, right = came
        here = slice(at, at + 64)
        there = slice(half * 256 + at, half * 256 + at + 64)
        return (mine[there] + recv4[there]) + (left[here] + right[here])

    came = lax.optimization_barrier((from_left0, from_right0))
    sums = tuple(first_sum(came, 0, at) for at in (0, 64, 128, 192))
    far0, far1, right0, right1 = lax.optimization_barrier(sums)
    via_left = round_ring(far0, 1, 1)
    via_right = round_ring(far1, 1, -1)
    next_left1 = round_ring(right1, 1, 1)
    came = lax.optimization_barrier((from_left1, from_right1))
    left0, left1, low, high = lax.optimization_barrier(tuple(first_sum(came, 1, at) for at in (0, 64, 128, 192)))
    next_right0 = round_ring(left0, 1, -1)
    next_left0 = round_ring(right0 + via_left, 1, 1)
    next_right1 = round_ring(left1 + via_right, 1, -1)
    low = low + next_left0 + next_right0
    high = high + next_left1 + next_right1
    rows = [low[:32], low[32:], high[:32], high[32:]]
    arrived = {}
    for k in (2, 1, 3):
        arrived[k] = round_ring(rows[k], 2, k)
    both = (rows[0] + arrived[1] + arrived[2] + arrived[3]) * (1.0 / total_cols)
    first = lax.axis_index(AX) * 16
    first_rows = (first - core * 128).astype(jnp.int32)
    parts = pauli_parts(jnp.stack([first_rows, core.astype(jnp.int32)]), both, pauli_x[None], pauli_z[None])
    parts = parts + swapped(parts)
    blocks = both.reshape(2, 16, 64, 16).transpose(2, 0, 3, 1).reshape(64, 512)
    message = jnp.concatenate([blocks, jnp.broadcast_to(parts, (64, 256))], 1)
    keep = lax.dynamic_slice_in_dim(both, core * 16, 16, 0)
    got = swapped(lax.dynamic_slice_in_dim(both, (1 - core) * 16, 16, 0))
    arrived = lax.all_to_all(message, SAME_CORE, split_axis=0, concat_axis=0, tiled=True)
    place = jnp.stack([first.astype(jnp.int32), core.astype(jnp.int32)])
    return tuple(densities(place, keep, got, arrived, pauli_x[None], pauli_z[None], pauli_phase[None]))


def solution(mesh):
    finer = Mesh(mesh.devices.reshape(mesh.shape["gx"], 2, 2, 4, 2), AX)
    in_specs = (P(None, AX, None), P(), P(), P())
    out_specs = (P(AX, None), P(AX, None), P())
    return jax.shard_map(on_device, mesh=finer, in_specs=in_specs, out_specs=out_specs, check_vma=False)
```
